32 devices in a mesh: band: 16 (over z, y, x), ch: 2 (over core).
Axes of the slice: x: 2, y: 2, z: 4, core: 2. Of those that a mesh axis runs over, the one named last changes fastest.
Arguments:
- grid_field: bfloat16 [100, 262144], P(None, 'band'), may hold values from -6 to 6
- band_points: int32 [16], P('band'), may hold values from 8192 to 16384
- block_ids: int32 [16, 16], P('band'), may hold values from 0 to 511, as said below
- block_count: int32 [16], P('band'), may hold values from 8 to 16
- block_weight: bfloat16 [16, 16, 256, 512], P('band'), may hold values from 0 to 0.039794922
- embed_weight: bfloat16 [100, 1024], P(None, 'ch'), may hold values from -0.3125 to 0.3125
- edge_src: int32 [81920], P('band'), may hold values from 0 to 4095, as said below
- edge_dst: int32 [81920], P('band'), may hold values from 0 to 4095, as said below
- edge_in_weight: bfloat16 [2, 1024, 1024], P(None, None, 'ch'), may hold values from -0.1875 to 0.1875
- edge_out_weight: bfloat16 [1024, 1024], P('ch'), may hold values from -0.0625 to 0.0625
- node_in_weight: bfloat16 [2, 1024, 1024], P(None, None, 'ch'), may hold values from -0.125 to 0.125
- node_out_weight: bfloat16 [1024, 1024], P('ch'), may hold values from -0.1875 to 0.1875
Outputs:
- node_state: bfloat16 [4096, 1024], P('band', 'ch')
The draws below stay inside these ranges and needn't reach their ends.
Inputs may be any that keep to these rules, and one draw needn't show every extreme that they name: For band b, block_ids[b, k] * 512 lies from max(b * 16384 - 16384 // 2, 0) to min((b + 1) * 16384 + 16384 // 2, 262144) - 512; both ends are named by every band; ids may repeat. `edge_src`: edge e belongs to band b = e // 5120; its source node lies in bands b - 1 to b + 1 of the mesh. `edge_dst`: edge e ends at a node of its band b = e // 5120.
All inputs are finite; a program needn't handle non-finite values.
Results may differ from the reference program's by a relative error of at most 0.015.
Values may be sent and summed in bfloat16 or wider, within the bound.
A program may use at most 64 MiB of HBM per device.

```python
import jax
import jax.numpy as jnp
from jax import lax

CIN = 100
H = 1024
PTS_DEV = 16384
NODE_DEV = 256
E_DEV = 5120
PBLK = 512
K = 16
POINTS = 262144
NODES = 4096
EDGES = 81920
N_BAND = 16


def draw_block_ids(key, part):
    sub_count = PTS_DEV // PBLK
    band_index = jnp.arange(N_BAND, dtype=jnp.int32)[:, None]
    lowest = jnp.maximum(band_index * sub_count - sub_count // 2, 0)
    highest = jnp.minimum((band_index + 1) * sub_count + sub_count // 2, N_BAND * sub_count)
    raw_bits = jax.random.randint(jax.random.fold_in(key, 11), (N_BAND, K), 0, 1 << 30)
    picked = lowest + raw_bits % (highest - lowest)
    slot_index = jnp.arange(K, dtype=jnp.int32)[None, :]
    picked = jnp.where(slot_index == 0, lowest, picked)
    picked = jnp.where(slot_index == 1, highest - 1, picked)
    return picked.astype(jnp.int32)


def draw_edge_src(key, part):
    edge_index = jnp.arange(EDGES, dtype=jnp.int32)
    band_index = edge_index // E_DEV
    lowest = jnp.maximum(band_index - 1, 0) * NODE_DEV
    highest = jnp.minimum(band_index + 2, N_BAND) * NODE_DEV
    return jax.random.randint(jax.random.fold_in(key, 21), (EDGES,), lowest, highest).astype(jnp.int32)


def draw_edge_dst(key, part):
    edge_index = jnp.arange(EDGES, dtype=jnp.int32)
    band_index = edge_index // E_DEV
    offset = jax.random.randint(jax.random.fold_in(key, 31), (EDGES,), 0, NODE_DEV)
    return (band_index * NODE_DEV + offset).astype(jnp.int32)


def set_ends(drawn, rng, low, high):
    spot = [jax.random.randint(jax.random.fold_in(rng, axis), (), 0, length) for axis, length in enumerate(drawn.shape)]
    longest = drawn.shape.index(max(drawn.shape))
    neighbour = spot[:longest] + [(spot[longest] + 1) % drawn.shape[longest]] + spot[longest + 1:]
    return drawn.at[tuple(spot)].set(low).at[tuple(neighbour)].set(high)


def block_levels(stream_key, extent, shards, low, top_value):
    level, own = 1.0, jax.random.fold_in(stream_key, 6)
    for dim, parts in shards:
        draws = jnp.exp(jax.random.uniform(jax.random.fold_in(own, dim), (parts,), jnp.float32, low / len(shards), top_value / len(shards)))
        level = level * jnp.repeat(draws, extent[dim] // parts).reshape([-1 if axis == dim else 1 for axis in range(len(extent))])
    return level


def bell_draw(stream_key, dims, scale, most, split=(), kind=jnp.bfloat16):
    entries = jax.random.normal(stream_key, dims, jnp.float32) * scale
    if len(split) > 0:
        entries = block_levels(stream_key, dims, split, -0.22, 0.18) * entries
    return jnp.clip(entries, min=-most, max=most).astype(kind)


def setup_inputs(seed: int = 0) -> dict:
    streams_of = jax.random.split(jax.random.key(seed), 13)
    grid_field = bell_draw(streams_of[0], (CIN, POINTS), 1.0, 6.0, ((1, 16),))
    band_points = set_ends(jax.random.randint(streams_of[1], (N_BAND,), PTS_DEV // 2, PTS_DEV + 1), jax.random.fold_in(streams_of[1], 1), PTS_DEV // 2, PTS_DEV).astype(jnp.int32)
    block_ids = draw_block_ids(jax.random.fold_in(streams_of[12], 71), 0)
    block_count = set_ends(jax.random.randint(streams_of[3], (N_BAND,), K // 2, K + 1), jax.random.fold_in(streams_of[3], 1), K // 2, K).astype(jnp.int32)
    block_weight = jnp.clip(0.039794922 * jax.random.uniform(streams_of[4], (N_BAND, K, NODE_DEV, PBLK), jnp.float32) ** block_levels(streams_of[4], (N_BAND, K, NODE_DEV, PBLK), ((0, 16),), -0.2, 0.2), 0.0, 0.039794922).astype(jnp.bfloat16)
    embed_weight = bell_draw(streams_of[5], (CIN, H), (4 * CIN) ** -0.5, 0.3125, ((1, 2),))
    edge_src = draw_edge_src(jax.random.fold_in(streams_of[12], 71), 0)
    edge_dst = draw_edge_dst(jax.random.fold_in(streams_of[12], 71), 0)
    edge_in_weight = bell_draw(streams_of[8], (2, H, H), H ** -0.5, 0.1875, ((2, 2),))
    edge_out_weight = bell_draw(streams_of[9], (H, H), (8 * H) ** -0.5, 0.0625, ((0, 2),))
    node_in_weight = bell_draw(streams_of[10], (2, H, H), (2 * H) ** -0.5, 0.125, ((2, 2),))
    node_out_weight = bell_draw(streams_of[11], (H, H), H ** -0.5, 0.1875, ((0, 2),))
    return {"grid_field": grid_field, "band_points": band_points, "block_ids": block_ids, "block_count": block_count, "block_weight": block_weight, "embed_weight": embed_weight, "edge_src": edge_src, "edge_dst": edge_dst, "edge_in_weight": edge_in_weight, "edge_out_weight": edge_out_weight, "node_in_weight": node_in_weight, "node_out_weight": node_out_weight}


def reference(grid_field, band_points, block_ids, block_count, block_weight, embed_weight, edge_src, edge_dst, edge_in_weight, edge_out_weight, node_in_weight, node_out_weight):
    column = jnp.arange(POINTS, dtype=jnp.int32)
    limit = band_points[column // PTS_DEV]
    live = jnp.where((column % PTS_DEV < limit)[None, :], grid_field, jnp.zeros_like(grid_field))
    tiles = live.reshape(CIN, POINTS // PBLK, PBLK)

    def remap_band(inputs):
        ids, count, weights = inputs
        blocks = jnp.take(tiles, ids, axis=1)
        live_mask = jnp.arange(K, dtype=jnp.int32) < count
        blocks = jnp.where(live_mask[None, :, None], blocks, jnp.zeros_like(blocks))
        summed = jnp.einsum("knp,ckp->nc", weights.astype(jnp.float32), blocks.astype(jnp.float32))
        return summed.astype(jnp.bfloat16)

    remapped = lax.map(remap_band, (block_ids, block_count, block_weight)).reshape(NODES, CIN)
    initial = jnp.dot(remapped, embed_weight, preferred_element_type=jnp.float32).astype(jnp.bfloat16)
    source_proj = jnp.dot(initial, edge_in_weight[0], preferred_element_type=jnp.float32).astype(jnp.bfloat16)
    target_proj = jnp.dot(initial, edge_in_weight[1], preferred_element_type=jnp.float32).astype(jnp.bfloat16)

    def band_messages(inputs):
        sources, targets = inputs
        pre_act = jnp.take(source_proj, sources, axis=0).astype(jnp.float32) + jnp.take(target_proj, targets, axis=0).astype(jnp.float32)
        edge_hidden = jax.nn.silu(pre_act).astype(jnp.bfloat16)
        messages = jnp.dot(edge_hidden, edge_out_weight, preferred_element_type=jnp.float32)
        return jax.ops.segment_sum(messages, targets % NODE_DEV, num_segments=NODE_DEV)

    aggregate = lax.map(band_messages, (edge_src.reshape(N_BAND, E_DEV), edge_dst.reshape(N_BAND, E_DEV)))
    aggregate = aggregate.reshape(NODES, H).astype(jnp.bfloat16)
    inner = jnp.dot(initial, node_in_weight[0], preferred_element_type=jnp.float32) + jnp.dot(aggregate, node_in_weight[1], preferred_element_type=jnp.float32)
    update = jax.nn.silu(inner).astype(jnp.bfloat16)
    result = initial.astype(jnp.float32) + jnp.dot(update, node_out_weight, preferred_element_type=jnp.float32)
    return result.astype(jnp.bfloat16)
```

```python
import functools

import jax
import jax.numpy as jnp
from jax import lax
from jax.experimental import pallas as pl
from jax.experimental.pallas import tpu as pltpu
from jax.sharding import PartitionSpec as P

MESH = pl.DeviceIdType.MESH
F32 = jnp.float32
BF16 = jnp.bfloat16
VMEM = pl.BlockSpec(memory_space=pltpu.VMEM)
SMEM = pl.BlockSpec(memory_space=pltpu.SMEM)
ANY = pl.BlockSpec(memory_space=pl.ANY)
LIMIT = 60 * 1024 * 1024


def buckets(most):
    pairs = [(3, 5), (4, 6), (5, 6), (5, 7), (6, 8), (8, 10)]
    return [p for p in pairs if max(p) < most] + [(most, most)]


def pack_kernel(half, width, need_ref, rank_ref, grid_ref, out_ref, sem):
    core = lax.axis_index("ch")

    def copy(side, i):
        block = half + i if side == 0 else i
        start = pl.multiple_of((block * 2 + core) * width, width)
        slot = rank_ref[side, i]
        return pltpu.make_async_copy(
            grid_ref.at[:, pl.ds(start, width)], out_ref.at[side, slot], sem.at[side, i]
        )

    for start in (True, False):
        for side in range(2):
            for i in range(half):
                @pl.when(need_ref[side, i] > 0)
                def _():
                    if start:
                        copy(side, i).start()
                    else:
                        copy(side, i).wait()


def exchange_kernel(n, low, high, pk, emb, eo, rv, emb_o, eo_o, send, recv):
    b = lax.axis_index("band")
    c = lax.axis_index("ch")
    up, down = jnp.minimum(b + 1, n - 1), jnp.maximum(b - 1, 0)
    has_up, has_down = b < n - 1, b > 0
    barrier = pltpu.get_barrier_semaphore()
    pl.semaphore_signal(barrier, inc=1, device_id=(b, 1 - c), device_id_type=MESH)

    @pl.when(has_up)
    def _():
        pl.semaphore_signal(barrier, inc=1, device_id=(up, c), device_id_type=MESH)

    @pl.when(has_down)
    def _():
        pl.semaphore_signal(barrier, inc=1, device_id=(down, c), device_id_type=MESH)

    pl.semaphore_wait(barrier, 1 + has_up.astype(jnp.int32) + has_down.astype(jnp.int32))

    def remote(src, dst, k, target):
        return pltpu.make_async_remote_copy(
            src_ref=src, dst_ref=dst, send_sem=send.at[k], recv_sem=recv.at[k],
            device_id=target, device_id_type=MESH,
        )

    fwd = remote(pk.at[0, pl.ds(0, low)], rv.at[0, pl.ds(0, low)], 0, (up, c))
    bwd = remote(pk.at[1, pl.ds(0, high)], rv.at[1, pl.ds(0, high)], 1, (down, c))
    own = [remote(emb, emb_o, 2, (b, 1 - c)), remote(eo, eo_o, 3, (b, 1 - c))]

    @pl.when(has_up)
    def _():
        fwd.start()

    @pl.when(has_down)
    def _():
        bwd.start()

    for one in own:
        one.start()
    for one in own:
        one.wait()

    @pl.when(has_up)
    def _():
        fwd.wait_send()
        bwd.wait_recv()

    @pl.when(has_down)
    def _():
        bwd.wait_send()
        fwd.wait_recv()


def remap_kernel(slots, width, kind_ref, index_ref, limit_ref, grid_ref, rv_ref, w_ref, out_ref, blk, wts, bsem, wsem):
    core = lax.axis_index("ch")
    off = pl.multiple_of(core * width, width)
    for k in range(slots):
        pltpu.make_async_copy(w_ref.at[k, :, pl.ds(off, width)], wts.at[k], wsem.at[k]).start()
    for k in range(slots):
        kind, index = kind_ref[k], index_ref[k]

        @pl.when(kind == 0)
        def _():
            start = pl.multiple_of((index * 2 + core) * width, width)
            pltpu.make_async_copy(grid_ref.at[:, pl.ds(start, width)], blk.at[k], bsem.at[k]).start()

        @pl.when(kind == 1)
        def _():
            pltpu.make_async_copy(rv_ref.at[0, index], blk.at[k], bsem.at[k]).start()

        @pl.when(kind == 2)
        def _():
            pltpu.make_async_copy(rv_ref.at[1, index], blk.at[k], bsem.at[k]).start()

    column = lax.broadcasted_iota(jnp.int32, blk.shape[1:], 1) + core * width
    total = jnp.zeros(out_ref.shape, F32)
    for k in range(slots):
        pltpu.make_async_copy(rv_ref.at[0, 0], blk.at[k], bsem.at[k]).wait()
        pltpu.make_async_copy(w_ref.at[k, :, pl.ds(off, width)], wts.at[k], wsem.at[k]).wait()
        block = blk[k]
        block = jnp.where(column < limit_ref[k], block, jnp.zeros_like(block))
        total += lax.dot_general(wts[k], block, (((1,), (1,)), ((), ())), preferred_element_type=F32)
    out_ref[...] = total


def share_kernel(n, part, out, other, ext, send, recv):
    b = lax.axis_index("band")
    c = lax.axis_index("ch")
    up, down = jnp.minimum(b + 1, n - 1), jnp.maximum(b - 1, 0)
    has_up, has_down = b < n - 1, b > 0
    barrier = pltpu.get_barrier_semaphore()
    pl.semaphore_signal(barrier, inc=1, device_id=(b, 1 - c), device_id_type=MESH)

    @pl.when(has_up)
    def _():
        pl.semaphore_signal(barrier, inc=1, device_id=(up, c), device_id_type=MESH)

    @pl.when(has_down)
    def _():
        pl.semaphore_signal(barrier, inc=1, device_id=(down, c), device_id_type=MESH)

    pl.semaphore_wait(barrier, 1 + has_up.astype(jnp.int32) + has_down.astype(jnp.int32))

    def remote(src, dst, k, target):
        return pltpu.make_async_remote_copy(
            src_ref=src, dst_ref=dst, send_sem=send.at[k], recv_sem=recv.at[k],
            device_id=target, device_id_type=MESH,
        )

    swap = remote(part, other, 0, (b, 1 - c))
    swap.start()
    swap.wait()
    ext[1] = (part[...] + other[...]).astype(BF16)
    fwd = remote(ext.at[1], ext.at[0], 1, (up, c))
    bwd = remote(ext.at[1], ext.at[2], 2, (down, c))

    @pl.when(has_up)
    def _():
        fwd.start()

    @pl.when(has_down)
    def _():
        bwd.start()

    @pl.when(has_up)
    def _():
        fwd.wait_send()
        bwd.wait_recv()

    @pl.when(has_down)
    def _():
        bwd.wait_send()
        fwd.wait_recv()

    out[...] = ext[...]

    @pl.when(b == 0)
    def _():
        out[0] = jnp.zeros(out.shape[1:], BF16)

    @pl.when(b == n - 1)
    def _():
        out[2] = jnp.zeros(out.shape[1:], BF16)


def silu(v):
    return (0.5 * v) * (1.0 + jnp.tanh(0.5 * v))


def edge_kernel(chunk, ext, emb, emb_o, src, dst, win, agg_out, init_out, init_s, table, acc):
    b = lax.axis_index("band")
    c = lax.axis_index("ch")
    nodes = ext.shape[1]
    half = emb.shape[1]
    rem = ext[...].reshape(3 * nodes, ext.shape[2])
    mine = pl.ds(pl.multiple_of(c * half, half), half)
    theirs = pl.ds(pl.multiple_of((1 - c) * half, half), half)
    init_s[:, mine] = jnp.dot(rem, emb[...], preferred_element_type=F32).astype(BF16)
    init_s[:, theirs] = jnp.dot(rem, emb_o[...], preferred_element_type=F32).astype(BF16)
    init_out[...] = init_s[nodes:2 * nodes, :]
    source = jnp.dot(init_s[...], win[0], preferred_element_type=F32)
    table[:, :3 * nodes] = source.T.astype(BF16)
    target = jnp.dot(init_s[nodes:2 * nodes, :], win[1], preferred_element_type=F32)
    table[:, 3 * nodes:] = target.T.astype(BF16)
    acc[...] = jnp.zeros_like(acc)
    one, zero = jnp.ones((), BF16), jnp.zeros((), BF16)

    def step(i, carry):
        cols = pl.ds(pl.multiple_of(i * chunk, chunk), chunk)
        s = src[:, cols] - (b - 1) * nodes
        d = dst[:, cols] - b * nodes
        from_src = lax.broadcasted_iota(jnp.int32, (3 * nodes, chunk), 0) == s
        from_dst = lax.broadcasted_iota(jnp.int32, (nodes, chunk), 0) == d
        hot_src = jnp.where(from_src, 1.0, 0.0).astype(BF16)
        hot_dst = jnp.where(from_dst, 1.0, 0.0).astype(BF16)
        pre = jnp.dot(table[...], jnp.concatenate([hot_src, hot_dst], axis=0), preferred_element_type=F32)
        hidden = silu(pre).astype(BF16)
        acc[...] += lax.dot_general(hot_dst, hidden, (((1,), (1,)), ((), ())), preferred_element_type=F32)
        return carry

    lax.fori_loop(0, src.shape[1] // chunk, step, 0)
    agg_out[...] = acc[...].astype(BF16)


def node_kernel(agg, init, eo, eo_o, nin, nout, out, agg_o, give, take, send, recv):
    b = lax.axis_index("band")
    c = lax.axis_index("ch")
    half = nin.shape[2]
    barrier = pltpu.get_barrier_semaphore()
    pl.semaphore_signal(barrier, inc=1, device_id=(b, 1 - c), device_id_type=MESH)
    pl.semaphore_wait(barrier, 1)

    def remote(src, dst, k):
        return pltpu.make_async_remote_copy(
            src_ref=src, dst_ref=dst, send_sem=send.at[k], recv_sem=recv.at[k],
            device_id=(b, 1 - c), device_id_type=MESH,
        )

    swap = remote(agg, agg_o, 0)
    swap.start()
    direct = jnp.dot(init[...], nin[0], preferred_element_type=F32)
    own = jnp.dot(agg[...], eo[...], preferred_element_type=F32)
    swap.wait()
    total = (own + jnp.dot(agg_o[...], eo_o[...], preferred_element_type=F32)).astype(BF16)
    update = silu(direct + jnp.dot(total, nin[1], preferred_element_type=F32)).astype(BF16)
    mine = pl.ds(pl.multiple_of(c * half, half), half)
    theirs = pl.ds(pl.multiple_of((1 - c) * half, half), half)
    give[...] = jnp.dot(update, nout[:, theirs], preferred_element_type=F32).astype(BF16)
    last = remote(give, take, 1)
    last.start()
    kept = init[:, mine].astype(F32) + jnp.dot(update, nout[:, mine], preferred_element_type=F32)
    last.wait()
    out[...] = (kept + take[...].astype(F32)).astype(BF16)


def on_device(
    grid_field, band_points, block_ids, block_count, block_weight, embed_weight,
    edge_src, edge_dst, edge_in_weight, edge_out_weight, node_in_weight, node_out_weight,
):
    n = lax.axis_size("band")
    b = lax.axis_index("band")
    channels, points = grid_field.shape
    slots, nodes, block_len = block_weight.shape[1:]
    sub = points // block_len
    half = sub // 2
    width = block_len // 2
    hid = embed_weight.shape[1]
    params = functools.partial(pltpu.CompilerParams, vmem_limit_bytes=LIMIT)

    meta = jnp.concatenate([block_ids[0], block_count, band_points])
    meta = lax.all_gather(meta, "band", axis=0)
    ids, count, live = meta[:, :slots], meta[:, slots], meta[:, slots + 1]
    bands = lax.iota(jnp.int32, n)
    rel = ids - bands[:, None] * sub + half
    used = lax.broadcasted_iota(jnp.int32, (n, slots), 1) < count[:, None]
    cand = lax.iota(jnp.int32, 2 * half)
    spot = jnp.where(cand < half, cand, cand + sub)
    below = jnp.concatenate([live[:1], live[:-1]])
    above = jnp.concatenate([live[1:], live[-1:]])
    start = jnp.where(cand < half, cand + half, cand - half) * block_len
    alive = jnp.where(cand[None] < half, start[None] < below[:, None], start[None] < above[:, None])
    named = jnp.any((rel[:, :, None] == spot[None, None, :]) & used[:, :, None], axis=1)
    need = (named & alive).astype(jnp.int32).reshape(n, 2, half)
    order = lax.iota(jnp.int32, half)
    rank = jnp.sum(jnp.where(order[None, :] < order[:, None], need[:, :, None, :], 0), axis=3)
    most = jnp.max(jnp.sum(need, axis=2), axis=0)
    sizes = buckets(half)
    choice = jnp.int32(0)
    for low, high in sizes[:-1]:
        choice += ((most[0] > low) | (most[1] > high)).astype(jnp.int32)

    up, down = jnp.minimum(b + 1, n - 1), jnp.maximum(b - 1, 0)
    pick = lambda a: jnp.stack([
        jnp.where(b < n - 1, lax.dynamic_index_in_dim(a, up, 0, False)[0], 0),
        jnp.where(b > 0, lax.dynamic_index_in_dim(a, down, 0, False)[1], 0),
    ])
    send_need, send_rank = pick(need), pick(rank)

    slot_shape = (2, half, channels, width)
    packed = pl.pallas_call(
        functools.partial(pack_kernel, half, width),
        out_shape=jax.ShapeDtypeStruct(slot_shape, BF16),
        in_specs=[SMEM, SMEM, ANY], out_specs=VMEM,
        scratch_shapes=[pltpu.SemaphoreType.DMA((2, half))],
        compiler_params=params(),
    )(send_need, send_rank, grid_field)

    def exchange(i, low, high, *args):
        return pl.pallas_call(
            functools.partial(exchange_kernel, n, low, high),
            out_shape=(
                jax.ShapeDtypeStruct(slot_shape, BF16),
                jax.ShapeDtypeStruct(embed_weight.shape, BF16),
                jax.ShapeDtypeStruct(edge_out_weight.shape, BF16),
            ),
            in_specs=[ANY] * 3, out_specs=(ANY,) * 3,
            scratch_shapes=[pltpu.SemaphoreType.DMA((4,)), pltpu.SemaphoreType.DMA((4,))],
            compiler_params=params(collective_id=i, has_side_effects=True),
        )(*args)

    received, embed_other, eo_other = lax.switch(
        choice,
        [functools.partial(exchange, i, low, high) for i, (low, high) in enumerate(sizes)],
        packed, embed_weight, edge_out_weight,
    )

    mine = lax.dynamic_index_in_dim(rel, b, 0, False)
    my_rank = lax.dynamic_index_in_dim(rank, b, 0, False)
    my_need = lax.dynamic_index_in_dim(need, b, 0, False)
    live_slot = lax.iota(jnp.int32, slots) < block_count[0]
    is_low, is_high = mine < half, mine >= half + sub
    side = jnp.where(is_low, mine, mine - sub)
    hit = side[:, None] == cand[None]
    far_index = jnp.sum(jnp.where(hit, my_rank.reshape(1, -1), 0), axis=1)
    far_need = jnp.sum(jnp.where(hit, my_need.reshape(1, -1), 0), axis=1) > 0
    far = (is_low | is_high) & far_need & live_slot
    kind = jnp.where(far, jnp.where(is_low, 1, 2), 0).astype(jnp.int32)
    local = jnp.clip(mine - half, 0, sub - 1)
    index = jnp.where(far, far_index, local).astype(jnp.int32)
    owner_live = jnp.where(is_low, live[down], jnp.where(is_high, live[up], band_points[0]))
    inner = jnp.where(is_low, mine + half, jnp.where(is_high, mine - half - sub, mine - half))
    limit = jnp.clip(owner_live - inner * block_len, 0, block_len)
    reachable = live_slot & (far | ~(is_low | is_high))
    limit = jnp.where(reachable, limit, 0).astype(jnp.int32)

    part = pl.pallas_call(
        functools.partial(remap_kernel, slots, width),
        out_shape=jax.ShapeDtypeStruct((nodes, channels), F32),
        in_specs=[SMEM, SMEM, SMEM, ANY, ANY, ANY], out_specs=VMEM,
        scratch_shapes=[
            pltpu.VMEM((slots, channels, width), BF16),
            pltpu.VMEM((slots, nodes, width), BF16),
            pltpu.SemaphoreType.DMA((slots,)),
            pltpu.SemaphoreType.DMA((slots,)),
        ],
        compiler_params=params(),
    )(kind, index, limit, grid_field, received, block_weight[0])

    ext = pl.pallas_call(
        functools.partial(share_kernel, n),
        out_shape=jax.ShapeDtypeStruct((3, nodes, channels), BF16),
        in_specs=[VMEM], out_specs=VMEM,
        scratch_shapes=[
            pltpu.VMEM((nodes, channels), F32),
            pltpu.VMEM((3, nodes, channels), BF16),
            pltpu.SemaphoreType.DMA((3,)), pltpu.SemaphoreType.DMA((3,)),
        ],
        compiler_params=params(collective_id=len(sizes), has_side_effects=True),
    )(part)

    edges = edge_src.shape[0]
    chunk = max(c for c in (512, 256, 128) if edges % c == 0)
    agg, initial = pl.pallas_call(
        functools.partial(edge_kernel, chunk),
        out_shape=(
            jax.ShapeDtypeStruct((nodes, hid), BF16),
            jax.ShapeDtypeStruct((nodes, 2 * hid), BF16),
        ),
        in_specs=[VMEM] * 6, out_specs=(VMEM, VMEM),
        scratch_shapes=[
            pltpu.VMEM((3 * nodes, 2 * hid), BF16),
            pltpu.VMEM((hid, 4 * nodes), BF16),
            pltpu.VMEM((nodes, hid), F32),
        ],
        compiler_params=params(),
    )(ext, embed_weight, embed_other, edge_src.reshape(1, -1), edge_dst.reshape(1, -1), edge_in_weight)

    return pl.pallas_call(
        node_kernel,
        out_shape=jax.ShapeDtypeStruct((nodes, hid), BF16),
        in_specs=[VMEM] * 6, out_specs=VMEM,
        scratch_shapes=[
            pltpu.VMEM((nodes, hid), BF16),
            pltpu.VMEM((nodes, hid), BF16),
            pltpu.VMEM((nodes, hid), BF16),
            pltpu.SemaphoreType.DMA((2,)), pltpu.SemaphoreType.DMA((2,)),
        ],
        compiler_params=params(collective_id=len(sizes) + 1, has_side_effects=True),
    )(agg, initial, edge_out_weight, eo_other, node_in_weight, node_out_weight)


def solution(mesh):
    return jax.shard_map(
        on_device,
        mesh=mesh,
        in_specs=(
            P(None, "band"), P("band"), P("band", None), P("band"),
            P("band", None, None, None), P(None, "ch"), P("band"), P("band"),
            P(None, None, "ch"), P("ch", None), P(None, None, "ch"), P("ch", None),
        ),
        out_specs=P("band", "ch"),
        check_vma=False,
    )
```

```python
import functools

import jax
import jax.numpy as jnp
from jax import lax
from jax.experimental import pallas as pl
from jax.experimental.pallas import tpu as pltpu
from jax.sharding import PartitionSpec as P

MESH = pl.DeviceIdType.MESH
F32 = jnp.float32
BF16 = jnp.bfloat16
VMEM = pl.BlockSpec(memory_space=pltpu.VMEM)
SMEM = pl.BlockSpec(memory_space=pltpu.SMEM)
ANY = pl.BlockSpec(memory_space=pl.ANY)
SMALL = 12 * 1024 * 1024
LARGE = 32 * 1024 * 1024


def buckets(most):
    pairs = [(3, 5), (4, 6), (5, 6), (5, 7), (6, 8), (8, 10)]
    return [p for p in pairs if max(p) < most] + [(most, most)]


def meta_kernel(n, slots, sub, block_len, sizes, ids, count, live, out, choice, row, rows, send, recv):
    b = lax.axis_index("band")
    c = lax.axis_index("ch")
    half = sub // 2
    row[:, :slots] = ids[...]
    row[:, slots:2 * slots] = jnp.full((1, slots), count[0], jnp.int32)
    row[:, 2 * slots:3 * slots] = jnp.full((1, slots), live[0], jnp.int32)
    row[:, 3 * slots:] = jnp.zeros((1, row.shape[1] - 3 * slots), jnp.int32)
    barrier = pltpu.get_barrier_semaphore()

    def greet(d, carry):
        pl.semaphore_signal(barrier, inc=1, device_id=(lax.rem(b + d, n), c), device_id_type=MESH)
        return carry

    lax.fori_loop(1, n, greet, 0)
    pl.semaphore_wait(barrier, n - 1)

    def copy(d):
        return pltpu.make_async_remote_copy(
            src_ref=row, dst_ref=rows.at[b], send_sem=send.at[d], recv_sem=recv.at[d],
            device_id=(lax.rem(b + d, n), c), device_id_type=MESH,
        )

    def begin(d, carry):
        copy(d).start()
        return carry

    def arrive(d, carry):
        pltpu.make_async_remote_copy(
            src_ref=row, dst_ref=rows.at[lax.rem(b + n - d, n)], send_sem=send.at[d], recv_sem=recv.at[d],
            device_id=(lax.rem(b + d, n), c), device_id_type=MESH,
        ).wait()
        return carry

    lax.fori_loop(1, n, begin, 0)
    rows[b] = row[...]
    lax.fori_loop(1, n, arrive, 0)
    out[...] = rows[...]
    every = rows[:, 0, :]
    named, most, points = every[:, :slots], every[:, slots:2 * slots], every[:, 2 * slots:2 * slots + 1]
    below = jnp.concatenate([points[:1], points[:-1]], axis=0)
    above = jnp.concatenate([points[1:], points[-1:]], axis=0)
    bands = lax.broadcasted_iota(jnp.int32, (n, 1), 0)
    rel = named - bands * sub + half
    rel = jnp.where(lax.broadcasted_iota(jnp.int32, (n, slots), 1) < most, rel, -1)
    counts = []
    for side in range(2):
        total = jnp.zeros((n, 1), F32)
        for i in range(half):
            spot = i if side == 0 else half + sub + i
            hit = jnp.max(jnp.where(rel == spot, 1.0, 0.0), axis=1, keepdims=True)
            alive = (half + i) * block_len < below if side == 0 else i * block_len < above
            total += jnp.where(alive, hit, 0.0)
        counts.append(jnp.max(total, axis=0, keepdims=True))
    pick = jnp.zeros((1, 1), jnp.int32)
    for low, high in sizes[:-1]:
        pick += jnp.where((counts[0] > low) | (counts[1] > high), 1, 0)
    choice[...] = jnp.broadcast_to(pick, choice.shape)


def pack_kernel(n, slots, sub, block_len, meta, grid_ref, out_ref, kind, index, limit, need, rank, mine, place, sem):
    b = lax.axis_index("band")
    core = lax.axis_index("ch")
    half = sub // 2
    width = block_len // 2

    def mark(side, band, owner, flags, ranks, active):
        for i in range(half):
            flags[side, i] = 0
        for k in range(slots):
            rel = meta[band, 0, k] - band * sub + half
            i = rel if side == 0 else rel - half - sub
            inner = rel + half if side == 0 else i
            good = (i >= 0) & (i < half) & (k < meta[band, 0, slots])
            good &= (inner * block_len < meta[owner, 0, 2 * slots]) & active
            i = jnp.clip(i, 0, half - 1)
            flags[side, i] = flags[side, i] | good.astype(jnp.int32)
        run = jnp.int32(0)
        for i in range(half):
            ranks[side, i] = run
            run += flags[side, i]

    up, down = jnp.minimum(b + 1, n - 1), jnp.maximum(b - 1, 0)

    def copy(side, i):
        block = half + i if side == 0 else i
        start = pl.multiple_of((block * 2 + core) * width, width)
        return pltpu.make_async_copy(
            grid_ref.at[:, pl.ds(start, width)], out_ref.at[side, rank[side, i]], sem.at[side, i]
        )

    def each(begin, side):
        for i in range(half):
            @pl.when(need[side, i] > 0)
            def _():
                if begin:
                    copy(side, i).start()
                else:
                    copy(side, i).wait()

    mark(0, up, b, need, rank, b < n - 1)
    each(True, 0)
    mark(1, down, b, need, rank, b > 0)
    each(True, 1)
    mark(0, b, down, mine, place, b > 0)
    mark(1, b, up, mine, place, b < n - 1)
    for k in range(slots):
        rel = meta[b, 0, k] - b * sub + half
        is_low, is_high = rel < half, rel >= half + sub
        side = is_high.astype(jnp.int32)
        i = jnp.clip(jnp.where(is_low, rel, rel - half - sub), 0, half - 1)
        used = k < meta[b, 0, slots]
        outside = is_low | is_high
        far = outside & used & (mine[side, i] > 0)
        owner = jnp.where(is_low, down, jnp.where(is_high, up, b))
        inner = jnp.where(is_low, rel + half, jnp.where(is_high, rel - half - sub, rel - half))
        span = jnp.clip(meta[owner, 0, 2 * slots] - inner * block_len, 0, block_len)
        kind[k] = jnp.where(far, 1 + side, 0)
        index[k] = jnp.where(far, place[side, i], jnp.clip(rel - half, 0, sub - 1))
        limit[k] = jnp.where(used & (far | ~outside), span, 0)
    each(False, 0)
    each(False, 1)


def exchange_kernel(n, low, high, pk, emb, eo, rv, emb_o, eo_o, send, recv):
    b = lax.axis_index("band")
    c = lax.axis_index("ch")
    up, down = jnp.minimum(b + 1, n - 1), jnp.maximum(b - 1, 0)
    has_up, has_down = b < n - 1, b > 0
    barrier = pltpu.get_barrier_semaphore()
    pl.semaphore_signal(barrier, inc=1, device_id=(b, 1 - c), device_id_type=MESH)

    @pl.when(has_up)
    def _():
        pl.semaphore_signal(barrier, inc=1, device_id=(up, c), device_id_type=MESH)

    @pl.when(has_down)
    def _():
        pl.semaphore_signal(barrier, inc=1, device_id=(down, c), device_id_type=MESH)

    pl.semaphore_wait(barrier, 1 + has_up.astype(jnp.int32) + has_down.astype(jnp.int32))

    def remote(src, dst, k, target):
        return pltpu.make_async_remote_copy(
            src_ref=src, dst_ref=dst, send_sem=send.at[k], recv_sem=recv.at[k],
            device_id=target, device_id_type=MESH,
        )

    fwd = remote(pk.at[0, pl.ds(0, low)], rv.at[0, pl.ds(0, low)], 0, (up, c))
    bwd = remote(pk.at[1, pl.ds(0, high)], rv.at[1, pl.ds(0, high)], 1, (down, c))
    own = [remote(emb, emb_o, 2, (b, 1 - c)), remote(eo, eo_o, 3, (b, 1 - c))]

    @pl.when(has_up)
    def _():
        fwd.start()

    @pl.when(has_down)
    def _():
        bwd.start()

    for one in own:
        one.start()
    for one in own:
        one.wait()

    @pl.when(has_up)
    def _():
        fwd.wait_send()
        bwd.wait_recv()

    @pl.when(has_down)
    def _():
        bwd.wait_send()
        fwd.wait_recv()


def remap_kernel(slots, width, kind_ref, index_ref, limit_ref, grid_ref, rv_ref, w_ref, out_ref, blk, wts, bsem, wsem):
    core = lax.axis_index("ch")
    off = pl.multiple_of(core * width, width)
    for k in range(slots):
        pltpu.make_async_copy(w_ref.at[k, :, pl.ds(off, width)], wts.at[k], wsem.at[k]).start()
    for k in range(slots):
        kind, index = kind_ref[k], index_ref[k]

        @pl.when(kind == 0)
        def _():
            start = pl.multiple_of((index * 2 + core) * width, width)
            pltpu.make_async_copy(grid_ref.at[:, pl.ds(start, width)], blk.at[k], bsem.at[k]).start()

        @pl.when(kind == 1)
        def _():
            pltpu.make_async_copy(rv_ref.at[0, index], blk.at[k], bsem.at[k]).start()

        @pl.when(kind == 2)
        def _():
            pltpu.make_async_copy(rv_ref.at[1, index], blk.at[k], bsem.at[k]).start()

    column = lax.broadcasted_iota(jnp.int32, blk.shape[1:], 1) + core * width
    total = jnp.zeros(out_ref.shape, F32)
    for k in range(slots):
        pltpu.make_async_copy(rv_ref.at[0, 0], blk.at[k], bsem.at[k]).wait()
        pltpu.make_async_copy(w_ref.at[k, :, pl.ds(off, width)], wts.at[k], wsem.at[k]).wait()
        block = blk[k]
        block = jnp.where(column < limit_ref[k], block, jnp.zeros_like(block))
        total += lax.dot_general(wts[k], block, (((1,), (1,)), ((), ())), preferred_element_type=F32)
    out_ref[...] = total


def share_kernel(n, part, out, other, ext, send, recv):
    b = lax.axis_index("band")
    c = lax.axis_index("ch")
    up, down = jnp.minimum(b + 1, n - 1), jnp.maximum(b - 1, 0)
    has_up, has_down = b < n - 1, b > 0
    barrier = pltpu.get_barrier_semaphore()
    pl.semaphore_signal(barrier, inc=1, device_id=(b, 1 - c), device_id_type=MESH)

    @pl.when(has_up)
    def _():
        pl.semaphore_signal(barrier, inc=1, device_id=(up, c), device_id_type=MESH)

    @pl.when(has_down)
    def _():
        pl.semaphore_signal(barrier, inc=1, device_id=(down, c), device_id_type=MESH)

    pl.semaphore_wait(barrier, 1 + has_up.astype(jnp.int32) + has_down.astype(jnp.int32))

    def remote(src, dst, k, target):
        return pltpu.make_async_remote_copy(
            src_ref=src, dst_ref=dst, send_sem=send.at[k], recv_sem=recv.at[k],
            device_id=target, device_id_type=MESH,
        )

    swap = remote(part, other, 0, (b, 1 - c))
    swap.start()
    swap.wait()
    ext[1] = (part[...] + other[...]).astype(BF16)
    fwd = remote(ext.at[1], ext.at[0], 1, (up, c))
    bwd = remote(ext.at[1], ext.at[2], 2, (down, c))

    @pl.when(has_up)
    def _():
        fwd.start()

    @pl.when(has_down)
    def _():
        bwd.start()

    @pl.when(has_up)
    def _():
        fwd.wait_send()
        bwd.wait_recv()

    @pl.when(has_down)
    def _():
        bwd.wait_send()
        fwd.wait_recv()

    out[...] = ext[...]

    @pl.when(b == 0)
    def _():
        out[0] = jnp.zeros(out.shape[1:], BF16)

    @pl.when(b == n - 1)
    def _():
        out[2] = jnp.zeros(out.shape[1:], BF16)


def silu(v):
    return (0.5 * v) * (1.0 + jnp.tanh(0.5 * v))


def edge_kernel(chunk, ext, emb, emb_o, src, dst, win, agg_out, init_out, init_s, table, acc):
    b = lax.axis_index("band")
    c = lax.axis_index("ch")
    nodes = ext.shape[1]
    half = emb.shape[1]
    rem = ext[...].reshape(3 * nodes, ext.shape[2])
    mine = pl.ds(pl.multiple_of(c * half, half), half)
    theirs = pl.ds(pl.multiple_of((1 - c) * half, half), half)
    init_s[:, mine] = jnp.dot(rem, emb[...], preferred_element_type=F32).astype(BF16)
    init_s[:, theirs] = jnp.dot(rem, emb_o[...], preferred_element_type=F32).astype(BF16)
    init_out[...] = init_s[nodes:2 * nodes, :]
    source = jnp.dot(init_s[...], win[0], preferred_element_type=F32)
    table[:, :3 * nodes] = source.T.astype(BF16)
    target = jnp.dot(init_s[nodes:2 * nodes, :], win[1], preferred_element_type=F32)
    table[:, 3 * nodes:] = target.T.astype(BF16)
    acc[...] = jnp.zeros_like(acc)
    one, zero = jnp.ones((), BF16), jnp.zeros((), BF16)

    def step(i, carry):
        cols = pl.ds(pl.multiple_of(i * chunk, chunk), chunk)
        s = src[:, cols] - (b - 1) * nodes
        d = dst[:, cols] - b * nodes
        from_src = lax.broadcasted_iota(jnp.int32, (3 * nodes, chunk), 0) == s
        from_dst = lax.broadcasted_iota(jnp.int32, (nodes, chunk), 0) == d
        hot_src = jnp.where(from_src, 1.0, 0.0).astype(BF16)
        hot_dst = jnp.where(from_dst, 1.0, 0.0).astype(BF16)
        pre = jnp.dot(table[...], jnp.concatenate([hot_src, hot_dst], axis=0), preferred_element_type=F32)
        hidden = silu(pre).astype(BF16)
        acc[...] += lax.dot_general(hot_dst, hidden, (((1,), (1,)), ((), ())), preferred_element_type=F32)
        return carry

    lax.fori_loop(0, src.shape[1] // chunk, step, 0, unroll=True)
    agg_out[...] = acc[...].astype(BF16)


def node_kernel(agg, init, eo, eo_o, nin, nout, out, agg_o, give, take, send, recv):
    b = lax.axis_index("band")
    c = lax.axis_index("ch")
    half = nin.shape[2]
    barrier = pltpu.get_barrier_semaphore()
    pl.semaphore_signal(barrier, inc=1, device_id=(b, 1 - c), device_id_type=MESH)
    pl.semaphore_wait(barrier, 1)

    def remote(src, dst, k):
        return pltpu.make_async_remote_copy(
            src_ref=src, dst_ref=dst, send_sem=send.at[k], recv_sem=recv.at[k],
            device_id=(b, 1 - c), device_id_type=MESH,
        )

    swap = remote(agg, agg_o, 0)
    swap.start()
    direct = jnp.dot(init[...], nin[0], preferred_element_type=F32)
    own = jnp.dot(agg[...], eo[...], preferred_element_type=F32)
    swap.wait()
    total = (own + jnp.dot(agg_o[...], eo_o[...], preferred_element_type=F32)).astype(BF16)
    update = silu(direct + jnp.dot(total, nin[1], preferred_element_type=F32)).astype(BF16)
    mine = pl.ds(pl.multiple_of(c * half, half), half)
    theirs = pl.ds(pl.multiple_of((1 - c) * half, half), half)
    give[...] = jnp.dot(update, nout[:, theirs], preferred_element_type=F32).astype(BF16)
    last = remote(give, take, 1)
    last.start()
    kept = init[:, mine].astype(F32) + jnp.dot(update, nout[:, mine], preferred_element_type=F32)
    last.wait()
    out[...] = (kept + take[...].astype(F32)).astype(BF16)


def on_device(
    grid_field, band_points, block_ids, block_count, block_weight, embed_weight,
    edge_src, edge_dst, edge_in_weight, edge_out_weight, node_in_weight, node_out_weight,
):
    n = lax.axis_size("band")
    channels, points = grid_field.shape
    slots, nodes, block_len = block_weight.shape[1:]
    sub = points // block_len
    half = sub // 2
    width = block_len // 2
    hid = embed_weight.shape[1]
    params = lambda limit, **kw: pltpu.CompilerParams(vmem_limit_bytes=limit, **kw)

    sizes = buckets(half)
    meta, choice = pl.pallas_call(
        functools.partial(meta_kernel, n, slots, sub, block_len, sizes),
        out_shape=(
            jax.ShapeDtypeStruct((n, 1, 128), jnp.int32),
            jax.ShapeDtypeStruct((1, 128), jnp.int32),
        ),
        in_specs=[VMEM, SMEM, SMEM], out_specs=(VMEM, VMEM),
        scratch_shapes=[
            pltpu.VMEM((1, 128), jnp.int32),
            pltpu.VMEM((n, 1, 128), jnp.int32),
            pltpu.SemaphoreType.DMA((n,)), pltpu.SemaphoreType.DMA((n,)),
        ],
        compiler_params=params(SMALL, collective_id=len(sizes) + 2, has_side_effects=True),
    )(block_ids, block_count, band_points)

    slot_shape = (2, half, channels, width)
    lists = jax.ShapeDtypeStruct((slots,), jnp.int32)
    table = pltpu.SMEM((2, half), jnp.int32)
    packed, kind, index, limit = pl.pallas_call(
        functools.partial(pack_kernel, n, slots, sub, block_len),
        out_shape=(jax.ShapeDtypeStruct(slot_shape, BF16), lists, lists, lists),
        in_specs=[SMEM, ANY], out_specs=(VMEM, SMEM, SMEM, SMEM),
        scratch_shapes=[table] * 4 + [pltpu.SemaphoreType.DMA((2, half))],
        compiler_params=params(SMALL),
    )(meta, grid_field)

    def exchange(i, low, high, *args):
        return pl.pallas_call(
            functools.partial(exchange_kernel, n, low, high),
            out_shape=(
                jax.ShapeDtypeStruct(slot_shape, BF16),
                jax.ShapeDtypeStruct(embed_weight.shape, BF16),
                jax.ShapeDtypeStruct(edge_out_weight.shape, BF16),
            ),
            in_specs=[ANY] * 3, out_specs=(ANY,) * 3,
            scratch_shapes=[pltpu.SemaphoreType.DMA((4,)), pltpu.SemaphoreType.DMA((4,))],
            compiler_params=params(SMALL, collective_id=i, has_side_effects=True),
        )(*args)

    received, embed_other, eo_other = lax.switch(
        choice[0, 0],
        [functools.partial(exchange, i, low, high) for i, (low, high) in enumerate(sizes)],
        packed, embed_weight, edge_out_weight,
    )

    part = pl.pallas_call(
        functools.partial(remap_kernel, slots, width),
        out_shape=jax.ShapeDtypeStruct((nodes, channels), F32),
        in_specs=[SMEM, SMEM, SMEM, ANY, ANY, ANY], out_specs=VMEM,
        scratch_shapes=[
            pltpu.VMEM((slots, channels, width), BF16),
            pltpu.VMEM((slots, nodes, width), BF16),
            pltpu.SemaphoreType.DMA((slots,)),
            pltpu.SemaphoreType.DMA((slots,)),
        ],
        compiler_params=params(SMALL),
    )(kind, index, limit, grid_field, received, block_weight[0])

    ext = pl.pallas_call(
        functools.partial(share_kernel, n),
        out_shape=jax.ShapeDtypeStruct((3, nodes, channels), BF16),
        in_specs=[VMEM], out_specs=VMEM,
        scratch_shapes=[
            pltpu.VMEM((nodes, channels), F32),
            pltpu.VMEM((3, nodes, channels), BF16),
            pltpu.SemaphoreType.DMA((3,)), pltpu.SemaphoreType.DMA((3,)),
        ],
        compiler_params=params(SMALL, collective_id=len(sizes), has_side_effects=True),
    )(part)

    edges = edge_src.shape[0]
    chunk = max(c for c in (512, 256, 128) if edges % c == 0)
    agg, initial = pl.pallas_call(
        functools.partial(edge_kernel, chunk),
        out_shape=(
            jax.ShapeDtypeStruct((nodes, hid), BF16),
            jax.ShapeDtypeStruct((nodes, 2 * hid), BF16),
        ),
        in_specs=[VMEM] * 6, out_specs=(VMEM, VMEM),
        scratch_shapes=[
            pltpu.VMEM((3 * nodes, 2 * hid), BF16),
            pltpu.VMEM((hid, 4 * nodes), BF16),
            pltpu.VMEM((nodes, hid), F32),
        ],
        compiler_params=params(LARGE),
    )(ext, embed_weight, embed_other, edge_src.reshape(1, -1), edge_dst.reshape(1, -1), edge_in_weight)

    return pl.pallas_call(
        node_kernel,
        out_shape=jax.ShapeDtypeStruct((nodes, hid), BF16),
        in_specs=[VMEM] * 6, out_specs=VMEM,
        scratch_shapes=[
            pltpu.VMEM((nodes, hid), BF16),
            pltpu.VMEM((nodes, hid), BF16),
            pltpu.VMEM((nodes, hid), BF16),
            pltpu.SemaphoreType.DMA((2,)), pltpu.SemaphoreType.DMA((2,)),
        ],
        compiler_params=params(LARGE, collective_id=len(sizes) + 1, has_side_effects=True),
    )(agg, initial, edge_out_weight, eo_other, node_in_weight, node_out_weight)


def solution(mesh):
    return jax.shard_map(
        on_device,
        mesh=mesh,
        in_specs=(
            P(None, "band"), P("band"), P("band", None), P("band"),
            P("band", None, None, None), P(None, "ch"), P("band"), P("band"),
            P(None, None, "ch"), P("ch", None), P(None, None, "ch"), P("ch", None),
        ),
        out_specs=P("band", "ch"),
        check_vma=False,
    )
```

```python
import functools

import jax
import jax.numpy as jnp
from jax import lax
from jax.experimental import pallas as pl
from jax.experimental.pallas import tpu as pltpu
from jax.sharding import PartitionSpec as P

MESH = pl.DeviceIdType.MESH
F32 = jnp.float32
BF16 = jnp.bfloat16
VMEM = pl.BlockSpec(memory_space=pltpu.VMEM)
SMEM = pl.BlockSpec(memory_space=pltpu.SMEM)
ANY = pl.BlockSpec(memory_space=pl.ANY)
SMALL = 12 * 1024 * 1024
LARGE = 40 * 1024 * 1024
UNROLL = 2


def buckets(most):
    pairs = [(4, 6), (5, 7), (7, 9)]
    return [p for p in pairs if max(p) < most] + [(most, most)]


def meta_kernel(n, slots, sub, block_len, sizes, ids, count, live, out, choice, row, rows, send, recv):
    b = lax.axis_index("band")
    c = lax.axis_index("ch")
    half = sub // 2
    row[:, :slots] = ids[...]
    row[:, slots:2 * slots] = jnp.full((1, slots), count[0], jnp.int32)
    row[:, 2 * slots:3 * slots] = jnp.full((1, slots), live[0], jnp.int32)
    row[:, 3 * slots:] = jnp.zeros((1, row.shape[1] - 3 * slots), jnp.int32)
    barrier = pltpu.get_barrier_semaphore()

    def greet(d, carry):
        pl.semaphore_signal(barrier, inc=1, device_id=(lax.rem(b + d, n), c), device_id_type=MESH)
        return carry

    lax.fori_loop(1, n, greet, 0)
    pl.semaphore_wait(barrier, n - 1)

    def copy(d):
        return pltpu.make_async_remote_copy(
            src_ref=row, dst_ref=rows.at[b], send_sem=send.at[d], recv_sem=recv.at[d],
            device_id=(lax.rem(b + d, n), c), device_id_type=MESH,
        )

    def begin(d, carry):
        copy(d).start()
        return carry

    def arrive(d, carry):
        pltpu.make_async_remote_copy(
            src_ref=row, dst_ref=rows.at[lax.rem(b + n - d, n)], send_sem=send.at[d], recv_sem=recv.at[d],
            device_id=(lax.rem(b + d, n), c), device_id_type=MESH,
        ).wait()
        return carry

    lax.fori_loop(1, n, begin, 0)
    rows[b] = row[...]
    lax.fori_loop(1, n, arrive, 0)
    out[...] = rows[...]
    every = rows[:, 0, :]
    named, most, points = every[:, :slots], every[:, slots:2 * slots], every[:, 2 * slots:2 * slots + 1]
    below = jnp.concatenate([points[:1], points[:-1]], axis=0)
    above = jnp.concatenate([points[1:], points[-1:]], axis=0)
    bands = lax.broadcasted_iota(jnp.int32, (n, 1), 0)
    rel = named - bands * sub + half
    rel = jnp.where(lax.broadcasted_iota(jnp.int32, (n, slots), 1) < most, rel, -1)
    counts = []
    for side in range(2):
        total = jnp.zeros((n, 1), F32)
        for i in range(half):
            spot = i if side == 0 else half + sub + i
            hit = jnp.max(jnp.where(rel == spot, 1.0, 0.0), axis=1, keepdims=True)
            alive = (half + i) * block_len < below if side == 0 else i * block_len < above
            total += jnp.where(alive, hit, 0.0)
        counts.append(jnp.max(total, axis=0, keepdims=True))
    pick = jnp.zeros((1, 1), jnp.int32)
    for low, high in sizes[:-1]:
        pick += jnp.where((counts[0] > low) | (counts[1] > high), 1, 0)
    choice[...] = jnp.broadcast_to(pick, choice.shape)


def pack_kernel(n, slots, sub, block_len, meta, grid_ref, out_ref, loc_ref, kind, index, limit, need, rank, mine, place, sem, lsem):
    b = lax.axis_index("band")
    core = lax.axis_index("ch")
    half = sub // 2
    width = block_len // 2

    def mark(side, band, owner, flags, ranks, active):
        for i in range(half):
            flags[side, i] = 0
        for k in range(slots):
            rel = meta[band, 0, k] - band * sub + half
            i = rel if side == 0 else rel - half - sub
            inner = rel + half if side == 0 else i
            good = (i >= 0) & (i < half) & (k < meta[band, 0, slots])
            good &= (inner * block_len < meta[owner, 0, 2 * slots]) & active
            i = jnp.clip(i, 0, half - 1)
            flags[side, i] = flags[side, i] | good.astype(jnp.int32)
        run = jnp.int32(0)
        for i in range(half):
            ranks[side, i] = run
            run += flags[side, i]

    up, down = jnp.minimum(b + 1, n - 1), jnp.maximum(b - 1, 0)

    def copy(side, i):
        block = half + i if side == 0 else i
        start = pl.multiple_of((block * 2 + core) * width, width)
        return pltpu.make_async_copy(
            grid_ref.at[:, pl.ds(start, width)], out_ref.at[side, rank[side, i]], sem.at[side, i]
        )

    def each(begin, side):
        for i in range(half):
            @pl.when(need[side, i] > 0)
            def _():
                if begin:
                    copy(side, i).start()
                else:
                    copy(side, i).wait()

    mark(0, up, b, need, rank, b < n - 1)
    each(True, 0)
    mark(1, down, b, need, rank, b > 0)
    each(True, 1)
    mark(0, b, down, mine, place, b > 0)
    mark(1, b, up, mine, place, b < n - 1)
    for k in range(slots):
        rel = meta[b, 0, k] - b * sub + half
        is_low, is_high = rel < half, rel >= half + sub
        side = is_high.astype(jnp.int32)
        i = jnp.clip(jnp.where(is_low, rel, rel - half - sub), 0, half - 1)
        used = k < meta[b, 0, slots]
        outside = is_low | is_high
        far = outside & used & (mine[side, i] > 0)
        owner = jnp.where(is_low, down, jnp.where(is_high, up, b))
        inner = jnp.where(is_low, rel + half, jnp.where(is_high, rel - half - sub, rel - half))
        span = jnp.clip(meta[owner, 0, 2 * slots] - inner * block_len, 0, block_len)
        kind[k] = jnp.where(far, 1 + side, 0)
        local = jnp.clip(rel - half, 0, sub - 1)
        index[k] = jnp.where(far, place[side, i], local)
        start = pl.multiple_of((local * 2 + core) * width, width)
        pltpu.make_async_copy(grid_ref.at[:, pl.ds(start, width)], loc_ref.at[k], lsem.at[k]).start()
        limit[k] = jnp.where(used & (far | ~outside), span, 0)
    each(False, 0)
    each(False, 1)
    for k in range(slots):
        pltpu.make_async_copy(grid_ref.at[:, pl.ds(0, width)], loc_ref.at[k], lsem.at[k]).wait()


def silu(v):
    return (0.5 * v) * (1.0 + jnp.tanh(0.5 * v))


def layer_kernel(
    n, low, high, chunk, kind, index, limit, pk, loc_h, w_h, emb_h, eo_h, win_h, nin_h, nout_h, src, dst, out,
    rlow, rhigh, loc, wts, blk, part, other, ext, emb, emb_o, eo, eo_o, win, nin, nout,
    init, table, acc, direct, agg, agg_o, give, take, wsem, lsem, send, recv,
):
    b = lax.axis_index("band")
    c = lax.axis_index("ch")
    slots, channels, width = loc.shape
    nodes = part.shape[0]
    half = emb.shape[1]
    up, down = jnp.minimum(b + 1, n - 1), jnp.maximum(b - 1, 0)
    has_up, has_down = b < n - 1, b > 0
    above, below, partner = (up, c), (down, c), (b, 1 - c)
    barrier = pltpu.get_barrier_semaphore()
    pl.semaphore_signal(barrier, inc=1, device_id=partner, device_id_type=MESH)

    @pl.when(has_up)
    def _():
        pl.semaphore_signal(barrier, inc=1, device_id=above, device_id_type=MESH)

    @pl.when(has_down)
    def _():
        pl.semaphore_signal(barrier, inc=1, device_id=below, device_id_type=MESH)

    pl.semaphore_wait(barrier, 1 + has_up.astype(jnp.int32) + has_down.astype(jnp.int32))

    def remote(source, target, k, device):
        return pltpu.make_async_remote_copy(
            src_ref=source, dst_ref=target, send_sem=send.at[k], recv_sem=recv.at[k],
            device_id=device, device_id_type=MESH,
        )

    def neighbours(fwd, bwd):
        def begin():
            pl.when(has_up)(fwd.start)
            pl.when(has_down)(bwd.start)

        def end():
            @pl.when(has_up)
            def _():
                fwd.wait_send()
                bwd.wait_recv()

            @pl.when(has_down)
            def _():
                bwd.wait_send()
                fwd.wait_recv()

        return begin, end

    blocks_begin, blocks_end = neighbours(
        remote(pk.at[0, pl.ds(0, low)], rlow, 0, above), remote(pk.at[1, pl.ds(0, high)], rhigh, 1, below)
    )
    blocks_begin()
    weights = [remote(emb_h, emb_o, 2, partner), remote(eo_h, eo_o, 3, partner)]
    for one in weights:
        one.start()
    off = pl.multiple_of(c * width, width)
    wcopies = [
        pltpu.make_async_copy(w_h.at[k, :, pl.ds(off, width)], wts.at[:, pl.ds(k * width, width)], wsem.at[k])
        for k in range(slots)
    ]
    local = [
        pltpu.make_async_copy(x, y, lsem.at[i])
        for i, (x, y) in enumerate(
            [(loc_h, loc), (emb_h, emb), (win_h, win), (eo_h, eo), (nin_h, nin), (nout_h, nout)]
        )
    ]
    for one in wcopies + local:
        one.start()

    @pl.when(b == 0)
    def _():
        rlow[...] = jnp.zeros_like(rlow)
        ext[0] = jnp.zeros((nodes, channels), BF16)

    @pl.when(b == n - 1)
    def _():
        rhigh[...] = jnp.zeros_like(rhigh)
        ext[2] = jnp.zeros((nodes, channels), BF16)

    for one in wcopies + local + weights:
        one.wait()
    blocks_end()

    column = lax.broadcasted_iota(jnp.int32, (channels, width), 1) + c * width
    for k in range(slots):
        which, i = kind[k], index[k]
        block = jnp.where(which == 1, rlow[jnp.clip(i, 0, low - 1)], loc[k])
        block = jnp.where(which == 2, rhigh[jnp.clip(i, 0, high - 1)], block)
        blk[:, k * width:(k + 1) * width] = jnp.where(column < limit[k], block, jnp.zeros_like(block))
    part[...] = lax.dot_general(wts[...], blk[...], (((1,), (1,)), ((), ())), preferred_element_type=F32)
    swap = remote(part, other, 4, partner)
    swap.start()
    swap.wait()
    ext[1] = (part[...] + other[...]).astype(BF16)
    rows_begin, rows_end = neighbours(remote(ext.at[1], ext.at[0], 5, above), remote(ext.at[1], ext.at[2], 6, below))
    rows_begin()

    mine = pl.ds(pl.multiple_of(c * half, half), half)
    theirs = pl.ds(pl.multiple_of((1 - c) * half, half), half)

    def project(i):
        rem = ext[i]
        init[i, :, mine] = jnp.dot(rem, emb[...], preferred_element_type=F32).astype(BF16)
        init[i, :, theirs] = jnp.dot(rem, emb_o[...], preferred_element_type=F32).astype(BF16)
        source = jnp.dot(init[i], win[0], preferred_element_type=F32)
        table[:, i * nodes:(i + 1) * nodes] = source.T.astype(BF16)

    project(1)
    target = jnp.dot(init[1], win[1], preferred_element_type=F32)
    table[:, 3 * nodes:] = target.T.astype(BF16)
    direct[...] = jnp.dot(init[1], nin[0], preferred_element_type=F32)
    acc[...] = jnp.zeros_like(acc)
    rows_end()
    project(0)
    project(2)

    def step(i, carry):
        cols = pl.ds(pl.multiple_of(i * chunk, chunk), chunk)
        s = src[:, cols] - (b - 1) * nodes
        d = dst[:, cols] - b * nodes
        from_src = lax.broadcasted_iota(jnp.int32, (3 * nodes, chunk), 0) == s
        from_dst = lax.broadcasted_iota(jnp.int32, (nodes, chunk), 0) == d
        hot_src = jnp.where(from_src, 1.0, 0.0).astype(BF16)
        hot_dst = jnp.where(from_dst, 1.0, 0.0).astype(BF16)
        pre = jnp.dot(table[...], jnp.concatenate([hot_src, hot_dst], axis=0), preferred_element_type=F32)
        hidden = silu(pre).astype(BF16)
        acc[...] += lax.dot_general(hot_dst, hidden, (((1,), (1,)), ((), ())), preferred_element_type=F32)
        return carry

    lax.fori_loop(0, src.shape[1] // chunk, step, 0, unroll=UNROLL)
    agg[...] = acc[...].astype(BF16)

    swap = remote(agg, agg_o, 7, partner)
    swap.start()
    own = jnp.dot(agg[...], eo[...], preferred_element_type=F32)
    swap.wait()
    total = (own + jnp.dot(agg_o[...], eo_o[...], preferred_element_type=F32)).astype(BF16)
    update = silu(direct[...] + jnp.dot(total, nin[1], preferred_element_type=F32)).astype(BF16)
    give[...] = jnp.dot(update, nout[:, theirs], preferred_element_type=F32).astype(BF16)
    last = remote(give, take, 8, partner)
    last.start()
    kept = init[1, :, mine].astype(F32) + jnp.dot(update, nout[:, mine], preferred_element_type=F32)
    last.wait()
    out[...] = (kept + take[...].astype(F32)).astype(BF16)


def on_device(
    grid_field, band_points, block_ids, block_count, block_weight, embed_weight,
    edge_src, edge_dst, edge_in_weight, edge_out_weight, node_in_weight, node_out_weight,
):
    n = lax.axis_size("band")
    channels, points = grid_field.shape
    slots, nodes, block_len = block_weight.shape[1:]
    sub = points // block_len
    half = sub // 2
    width = block_len // 2
    hid = embed_weight.shape[1]
    params = lambda limit, **kw: pltpu.CompilerParams(vmem_limit_bytes=limit, **kw)

    sizes = buckets(half)
    meta, choice = pl.pallas_call(
        functools.partial(meta_kernel, n, slots, sub, block_len, sizes),
        out_shape=(
            jax.ShapeDtypeStruct((n, 1, 128), jnp.int32),
            jax.ShapeDtypeStruct((1, 128), jnp.int32),
        ),
        in_specs=[VMEM, SMEM, SMEM], out_specs=(VMEM, VMEM),
        scratch_shapes=[
            pltpu.VMEM((1, 128), jnp.int32),
            pltpu.VMEM((n, 1, 128), jnp.int32),
            pltpu.SemaphoreType.DMA((n,)), pltpu.SemaphoreType.DMA((n,)),
        ],
        compiler_params=params(SMALL, collective_id=len(sizes) + 2, has_side_effects=True),
    )(block_ids, block_count, band_points)

    slot_shape = (2, half, channels, width)
    lists = jax.ShapeDtypeStruct((slots,), jnp.int32)
    table = pltpu.SMEM((2, half), jnp.int32)
    packed, local, kind, index, limit = pl.pallas_call(
        functools.partial(pack_kernel, n, slots, sub, block_len),
        out_shape=(jax.ShapeDtypeStruct(slot_shape, BF16), jax.ShapeDtypeStruct((slots, channels, width), BF16), lists, lists, lists),
        in_specs=[SMEM, ANY], out_specs=(VMEM, VMEM, SMEM, SMEM, SMEM),
        scratch_shapes=[table] * 4 + [pltpu.SemaphoreType.DMA((2, half)), pltpu.SemaphoreType.DMA((slots,))],
        compiler_params=params(SMALL),
    )(meta, grid_field)

    edges = edge_src.shape[0]
    chunk = max(c for c in (512, 256, 128) if edges % c == 0)

    def layer(i, low, high, *args):
        bf = lambda *shape: pltpu.VMEM(shape, BF16)
        f32 = lambda *shape: pltpu.VMEM(shape, F32)
        return pl.pallas_call(
            functools.partial(layer_kernel, n, low, high, chunk),
            out_shape=jax.ShapeDtypeStruct((nodes, hid), BF16),
            in_specs=[SMEM] * 3 + [ANY] * 8 + [VMEM] * 2, out_specs=VMEM,
            scratch_shapes=[
                bf(low, channels, width), bf(high, channels, width), bf(slots, channels, width),
                bf(nodes, slots * width), bf(channels, slots * width),
                f32(nodes, channels), f32(nodes, channels), bf(3, nodes, channels),
                bf(channels, hid), bf(channels, hid), bf(hid, 2 * hid), bf(hid, 2 * hid),
                bf(2, 2 * hid, hid), bf(2, 2 * hid, hid), bf(hid, 2 * hid),
                bf(3, nodes, 2 * hid), bf(hid, 4 * nodes), f32(nodes, hid), f32(nodes, hid),
                bf(nodes, hid), bf(nodes, hid), bf(nodes, hid), bf(nodes, hid),
                pltpu.SemaphoreType.DMA((slots,)), pltpu.SemaphoreType.DMA((6,)),
                pltpu.SemaphoreType.DMA((9,)), pltpu.SemaphoreType.DMA((9,)),
            ],
            compiler_params=params(LARGE, collective_id=i, has_side_effects=True),
        )(*args)

    return lax.switch(
        choice[0, 0],
        [functools.partial(layer, i, low, high) for i, (low, high) in enumerate(sizes)],
        kind, index, limit, packed, local, block_weight[0], embed_weight, edge_out_weight,
        edge_in_weight, node_in_weight, node_out_weight, edge_src.reshape(1, -1), edge_dst.reshape(1, -1),
    )


def solution(mesh):
    return jax.shard_map(
        on_device,
        mesh=mesh,
        in_specs=(
            P(None, "band"), P("band"), P("band", None), P("band"),
            P("band", None, None, None), P(None, "ch"), P("band"), P("band"),
            P(None, None, "ch"), P("ch", None), P(None, None, "ch"), P("ch", None),
        ),
        out_specs=P("band", "ch"),
        check_vma=False,
    )
```

```python
import functools

import jax
import jax.numpy as jnp
from jax import lax
from jax.experimental import pallas as pl
from jax.experimental.pallas import tpu as pltpu
from jax.sharding import PartitionSpec as P

MESH = pl.DeviceIdType.MESH
F32 = jnp.float32
BF16 = jnp.bfloat16
VMEM = pl.BlockSpec(memory_space=pltpu.VMEM)
SMEM = pl.BlockSpec(memory_space=pltpu.SMEM)
ANY = pl.BlockSpec(memory_space=pl.ANY)
HBM = pl.BlockSpec(memory_space=pltpu.HBM)
SMALL = 12 * 1024 * 1024
LARGE = 40 * 1024 * 1024
UNROLL = 2


def buckets(most):
    pairs = [(4, 6), (5, 7), (7, 9)]
    return [p for p in pairs if max(p) < most] + [(most, most)]


def meta_kernel(n, slots, sub, block_len, sizes, ids, count, live, out, choice, row, rows, send, recv):
    b = lax.axis_index("band")
    c = lax.axis_index("ch")
    half = sub // 2
    row[:, :slots] = ids[...]
    row[:, slots:2 * slots] = jnp.full((1, slots), count[0], jnp.int32)
    row[:, 2 * slots:3 * slots] = jnp.full((1, slots), live[0], jnp.int32)
    row[:, 3 * slots:] = jnp.zeros((1, row.shape[1] - 3 * slots), jnp.int32)
    barrier = pltpu.get_barrier_semaphore()

    def greet(d, carry):
        pl.semaphore_signal(barrier, inc=1, device_id=(lax.rem(b + d, n), c), device_id_type=MESH)
        return carry

    lax.fori_loop(1, n, greet, 0)
    pl.semaphore_wait(barrier, n - 1)

    def copy(d):
        return pltpu.make_async_remote_copy(
            src_ref=row, dst_ref=rows.at[b], send_sem=send.at[d], recv_sem=recv.at[d],
            device_id=(lax.rem(b + d, n), c), device_id_type=MESH,
        )

    def begin(d, carry):
        copy(d).start()
        return carry

    def arrive(d, carry):
        pltpu.make_async_remote_copy(
            src_ref=row, dst_ref=rows.at[lax.rem(b + n - d, n)], send_sem=send.at[d], recv_sem=recv.at[d],
            device_id=(lax.rem(b + d, n), c), device_id_type=MESH,
        ).wait()
        return carry

    lax.fori_loop(1, n, begin, 0)
    rows[b] = row[...]
    lax.fori_loop(1, n, arrive, 0)
    out[...] = rows[...]
    every = rows[:, 0, :]
    named, most, points = every[:, :slots], every[:, slots:2 * slots], every[:, 2 * slots:2 * slots + 1]
    below = jnp.concatenate([points[:1], points[:-1]], axis=0)
    above = jnp.concatenate([points[1:], points[-1:]], axis=0)
    bands = lax.broadcasted_iota(jnp.int32, (n, 1), 0)
    rel = named - bands * sub + half
    rel = jnp.where(lax.broadcasted_iota(jnp.int32, (n, slots), 1) < most, rel, -1)
    counts = []
    for side in range(2):
        total = jnp.zeros((n, 1), F32)
        for i in range(half):
            spot = i if side == 0 else half + sub + i
            hit = jnp.max(jnp.where(rel == spot, 1.0, 0.0), axis=1, keepdims=True)
            alive = (half + i) * block_len < below if side == 0 else i * block_len < above
            total += jnp.where(alive, hit, 0.0)
        counts.append(jnp.max(total, axis=0, keepdims=True))
    pick = jnp.zeros((1, 1), jnp.int32)
    for low, high in sizes[:-1]:
        pick += jnp.where((counts[0] > low) | (counts[1] > high), 1, 0)
    choice[...] = jnp.broadcast_to(pick, choice.shape)


def pack_kernel(n, slots, sub, block_len, meta, grid_ref, out_ref, kind, index, limit, need, rank, mine, place, sem):
    b = lax.axis_index("band")
    core = lax.axis_index("ch")
    half = sub // 2
    width = block_len // 2

    def mark(side, band, owner, flags, ranks, active):
        for i in range(half):
            flags[side, i] = 0
        for k in range(slots):
            rel = meta[band, 0, k] - band * sub + half
            i = rel if side == 0 else rel - half - sub
            inner = rel + half if side == 0 else i
            good = (i >= 0) & (i < half) & (k < meta[band, 0, slots])
            good &= (inner * block_len < meta[owner, 0, 2 * slots]) & active
            i = jnp.clip(i, 0, half - 1)
            flags[side, i] = flags[side, i] | good.astype(jnp.int32)
        run = jnp.int32(0)
        for i in range(half):
            ranks[side, i] = run
            run += flags[side, i]

    up, down = jnp.minimum(b + 1, n - 1), jnp.maximum(b - 1, 0)

    def copy(side, i):
        block = half + i if side == 0 else i
        start = pl.multiple_of((block * 2 + core) * width, width)
        return pltpu.make_async_copy(
            grid_ref.at[:, pl.ds(start, width)], out_ref.at[side, rank[side, i]], sem.at[side, i]
        )

    def each(begin, side):
        for i in range(half):
            @pl.when(need[side, i] > 0)
            def _():
                if begin:
                    copy(side, i).start()
                else:
                    copy(side, i).wait()

    mark(0, up, b, need, rank, b < n - 1)
    each(True, 0)
    mark(1, down, b, need, rank, b > 0)
    each(True, 1)
    mark(0, b, down, mine, place, b > 0)
    mark(1, b, up, mine, place, b < n - 1)
    for k in range(slots):
        rel = meta[b, 0, k] - b * sub + half
        is_low, is_high = rel < half, rel >= half + sub
        side = is_high.astype(jnp.int32)
        i = jnp.clip(jnp.where(is_low, rel, rel - half - sub), 0, half - 1)
        used = k < meta[b, 0, slots]
        outside = is_low | is_high
        far = outside & used & (mine[side, i] > 0)
        owner = jnp.where(is_low, down, jnp.where(is_high, up, b))
        inner = jnp.where(is_low, rel + half, jnp.where(is_high, rel - half - sub, rel - half))
        span = jnp.clip(meta[owner, 0, 2 * slots] - inner * block_len, 0, block_len)
        kind[k] = jnp.where(far, 1 + side, 0)
        local = jnp.clip(rel - half, 0, sub - 1)
        index[k] = jnp.where(far, place[side, i], local)
        limit[k] = jnp.where(used & (far | ~outside), span, 0)
    each(False, 0)
    each(False, 1)


def silu(v):
    return (0.5 * v) * (1.0 + jnp.tanh(0.5 * v))


def layer_kernel(
    n, low, high, chunk, kind, index, limit, pk, grid_h, w_h, emb_h, eo_h, win_h, nin_h, nout_h, src, dst, out,
    rlow, rhigh, loc, wts, blk, part, other, ext, emb, emb_o, eo, eo_o, win, nin, nout,
    init, table, acc, direct, agg, agg_o, give, take, wsem, gsem, lsem, send, recv,
):
    b = lax.axis_index("band")
    c = lax.axis_index("ch")
    sub, channels, width = loc.shape
    slots = w_h.shape[0]
    nodes = part.shape[0]
    half = emb.shape[1]
    up, down = jnp.minimum(b + 1, n - 1), jnp.maximum(b - 1, 0)
    has_up, has_down = b < n - 1, b > 0
    above, below, partner = (up, c), (down, c), (b, 1 - c)
    barrier = pltpu.get_barrier_semaphore()
    pl.semaphore_signal(barrier, inc=1, device_id=partner, device_id_type=MESH)

    @pl.when(has_up)
    def _():
        pl.semaphore_signal(barrier, inc=1, device_id=above, device_id_type=MESH)

    @pl.when(has_down)
    def _():
        pl.semaphore_signal(barrier, inc=1, device_id=below, device_id_type=MESH)

    pl.semaphore_wait(barrier, 1 + has_up.astype(jnp.int32) + has_down.astype(jnp.int32))

    def remote(source, target, k, device):
        return pltpu.make_async_remote_copy(
            src_ref=source, dst_ref=target, send_sem=send.at[k], recv_sem=recv.at[k],
            device_id=device, device_id_type=MESH,
        )

    def neighbours(fwd, bwd):
        def begin():
            pl.when(has_up)(fwd.start)
            pl.when(has_down)(bwd.start)

        def end():
            @pl.when(has_up)
            def _():
                fwd.wait_send()
                bwd.wait_recv()

            @pl.when(has_down)
            def _():
                bwd.wait_send()
                fwd.wait_recv()

        return begin, end

    blocks_begin, blocks_end = neighbours(
        remote(pk.at[0, pl.ds(0, low)], rlow, 0, above), remote(pk.at[1, pl.ds(0, high)], rhigh, 1, below)
    )
    blocks_begin()
    weights = [remote(emb_h, emb_o, 2, partner), remote(eo_h, eo_o, 3, partner)]
    for one in weights:
        one.start()
    off = pl.multiple_of(c * width, width)
    wcopies = [
        pltpu.make_async_copy(w_h.at[k, :, pl.ds(off, width)], wts.at[:, pl.ds(k * width, width)], wsem.at[k])
        for k in range(slots)
    ]
    gcopies = [
        pltpu.make_async_copy(
            grid_h.at[:, pl.ds(pl.multiple_of((2 * i + c) * width, width), width)], loc.at[i], gsem.at[i]
        )
        for i in range(sub)
    ]
    local = [
        pltpu.make_async_copy(x, y, lsem.at[i])
        for i, (x, y) in enumerate(
            [(emb_h, emb), (win_h, win), (eo_h, eo), (nin_h, nin), (nout_h, nout)]
        )
    ]
    for one in wcopies + gcopies + local:
        one.start()

    @pl.when(b == 0)
    def _():
        rlow[...] = jnp.zeros_like(rlow)
        ext[0] = jnp.zeros((nodes, channels), BF16)

    @pl.when(b == n - 1)
    def _():
        rhigh[...] = jnp.zeros_like(rhigh)
        ext[2] = jnp.zeros((nodes, channels), BF16)

    for one in wcopies + gcopies + local + weights:
        one.wait()
    blocks_end()

    column = lax.broadcasted_iota(jnp.int32, (channels, width), 1) + c * width
    for k in range(slots):
        which, i = kind[k], index[k]
        block = jnp.where(which == 1, rlow[jnp.clip(i, 0, low - 1)], loc[i])
        block = jnp.where(which == 2, rhigh[jnp.clip(i, 0, high - 1)], block)
        blk[:, k * width:(k + 1) * width] = jnp.where(column < limit[k], block, jnp.zeros_like(block))
    part[...] = lax.dot_general(wts[...], blk[...], (((1,), (1,)), ((), ())), preferred_element_type=F32)
    swap = remote(part, other, 4, partner)
    swap.start()
    swap.wait()
    ext[1] = (part[...] + other[...]).astype(BF16)
    rows_begin, rows_end = neighbours(remote(ext.at[1], ext.at[0], 5, above), remote(ext.at[1], ext.at[2], 6, below))
    rows_begin()

    mine = pl.ds(pl.multiple_of(c * half, half), half)
    theirs = pl.ds(pl.multiple_of((1 - c) * half, half), half)

    def project(i):
        rem = ext[i]
        init[i, :, mine] = jnp.dot(rem, emb[...], preferred_element_type=F32).astype(BF16)
        init[i, :, theirs] = jnp.dot(rem, emb_o[...], preferred_element_type=F32).astype(BF16)
        source = jnp.dot(init[i], win[0], preferred_element_type=F32)
        table[:, i * nodes:(i + 1) * nodes] = source.T.astype(BF16)

    project(1)
    target = jnp.dot(init[1], win[1], preferred_element_type=F32)
    table[:, 3 * nodes:] = target.T.astype(BF16)
    direct[...] = jnp.dot(init[1], nin[0], preferred_element_type=F32)
    acc[...] = jnp.zeros_like(acc)
    rows_end()
    project(0)
    project(2)

    def step(i, carry):
        cols = pl.ds(pl.multiple_of(i * chunk, chunk), chunk)
        s = src[:, cols] - (b - 1) * nodes
        d = dst[:, cols] - b * nodes
        from_src = lax.broadcasted_iota(jnp.int32, (3 * nodes, chunk), 0) == s
        from_dst = lax.broadcasted_iota(jnp.int32, (nodes, chunk), 0) == d
        hot_src = jnp.where(from_src, 1.0, 0.0).astype(BF16)
        hot_dst = jnp.where(from_dst, 1.0, 0.0).astype(BF16)
        pre = jnp.dot(table[...], jnp.concatenate([hot_src, hot_dst], axis=0), preferred_element_type=F32)
        hidden = silu(pre).astype(BF16)
        acc[...] += lax.dot_general(hot_dst, hidden, (((1,), (1,)), ((), ())), preferred_element_type=F32)
        return carry

    lax.fori_loop(0, src.shape[1] // chunk, step, 0, unroll=UNROLL)
    agg[...] = acc[...].astype(BF16)

    swap = remote(agg, agg_o, 7, partner)
    swap.start()
    own = jnp.dot(agg[...], eo[...], preferred_element_type=F32)
    swap.wait()
    total = (own + jnp.dot(agg_o[...], eo_o[...], preferred_element_type=F32)).astype(BF16)
    update = silu(direct[...] + jnp.dot(total, nin[1], preferred_element_type=F32)).astype(BF16)
    give[...] = jnp.dot(update, nout[:, theirs], preferred_element_type=F32).astype(BF16)
    last = remote(give, take, 8, partner)
    last.start()
    kept = init[1, :, mine].astype(F32) + jnp.dot(update, nout[:, mine], preferred_element_type=F32)
    last.wait()
    out[...] = (kept + take[...].astype(F32)).astype(BF16)


def on_device(
    grid_field, band_points, block_ids, block_count, block_weight, embed_weight,
    edge_src, edge_dst, edge_in_weight, edge_out_weight, node_in_weight, node_out_weight,
):
    n = lax.axis_size("band")
    channels, points = grid_field.shape
    slots, nodes, block_len = block_weight.shape[1:]
    sub = points // block_len
    half = sub // 2
    width = block_len // 2
    hid = embed_weight.shape[1]
    params = lambda limit, **kw: pltpu.CompilerParams(vmem_limit_bytes=limit, **kw)

    sizes = buckets(half)
    meta, choice = pl.pallas_call(
        functools.partial(meta_kernel, n, slots, sub, block_len, sizes),
        out_shape=(
            jax.ShapeDtypeStruct((n, 1, 128), jnp.int32),
            jax.ShapeDtypeStruct((1, 128), jnp.int32),
        ),
        in_specs=[VMEM, SMEM, SMEM], out_specs=(VMEM, VMEM),
        scratch_shapes=[
            pltpu.VMEM((1, 128), jnp.int32),
            pltpu.VMEM((n, 1, 128), jnp.int32),
            pltpu.SemaphoreType.DMA((n,)), pltpu.SemaphoreType.DMA((n,)),
        ],
        compiler_params=params(SMALL, collective_id=len(sizes) + 2, has_side_effects=True),
    )(block_ids, block_count, band_points)

    slot_shape = (2, half, channels, width)
    lists = jax.ShapeDtypeStruct((slots,), jnp.int32)
    table = pltpu.SMEM((2, half), jnp.int32)
    packed, kind, index, limit = pl.pallas_call(
        functools.partial(pack_kernel, n, slots, sub, block_len),
        out_shape=(jax.ShapeDtypeStruct(slot_shape, BF16), lists, lists, lists),
        in_specs=[SMEM, HBM], out_specs=(VMEM, SMEM, SMEM, SMEM),
        scratch_shapes=[table] * 4 + [pltpu.SemaphoreType.DMA((2, half))],
        compiler_params=params(SMALL),
    )(meta, grid_field)

    edges = edge_src.shape[0]
    chunk = max(c for c in (512, 256, 128) if edges % c == 0)

    def layer(i, low, high, *args):
        bf = lambda *shape: pltpu.VMEM(shape, BF16)
        f32 = lambda *shape: pltpu.VMEM(shape, F32)
        return pl.pallas_call(
            functools.partial(layer_kernel, n, low, high, chunk),
            out_shape=jax.ShapeDtypeStruct((nodes, hid), BF16),
            in_specs=[SMEM] * 3 + [ANY] + [HBM] * 7 + [VMEM] * 2, out_specs=VMEM,
            scratch_shapes=[
                bf(low, channels, width), bf(high, channels, width), bf(sub, channels, width),
                bf(nodes, slots * width), bf(channels, slots * width),
                f32(nodes, channels), f32(nodes, channels), bf(3, nodes, channels),
                bf(channels, hid), bf(channels, hid), bf(hid, 2 * hid), bf(hid, 2 * hid),
                bf(2, 2 * hid, hid), bf(2, 2 * hid, hid), bf(hid, 2 * hid),
                bf(3, nodes, 2 * hid), bf(hid, 4 * nodes), f32(nodes, hid), f32(nodes, hid),
                bf(nodes, hid), bf(nodes, hid), bf(nodes, hid), bf(nodes, hid),
                pltpu.SemaphoreType.DMA((slots,)), pltpu.SemaphoreType.DMA((sub,)), pltpu.SemaphoreType.DMA((5,)),
                pltpu.SemaphoreType.DMA((9,)), pltpu.SemaphoreType.DMA((9,)),
            ],
            compiler_params=params(LARGE, collective_id=i, has_side_effects=True),
        )(*args)

    return lax.switch(
        choice[0, 0],
        [functools.partial(layer, i, low, high) for i, (low, high) in enumerate(sizes)],
        kind, index, limit, packed, grid_field, block_weight.reshape(block_weight.shape[1:]), embed_weight, edge_out_weight,
        edge_in_weight, node_in_weight, node_out_weight, edge_src.reshape(1, -1), edge_dst.reshape(1, -1),
    )


def solution(mesh):
    return jax.shard_map(
        on_device,
        mesh=mesh,
        in_specs=(
            P(None, "band"), P("band"), P("band", None), P("band"),
            P("band", None, None, None), P(None, "ch"), P("band"), P("band"),
            P(None, None, "ch"), P("ch", None), P(None, None, "ch"), P("ch", None),
        ),
        out_specs=P("band", "ch"),
        check_vma=False,
    )
```

```python
import functools

import jax
import jax.numpy as jnp
from jax import lax
from jax.experimental import pallas as pl
from jax.experimental.pallas import tpu as pltpu
from jax.sharding import PartitionSpec as P

MESH = pl.DeviceIdType.MESH
F32 = jnp.float32
BF16 = jnp.bfloat16
VMEM = pl.BlockSpec(memory_space=pltpu.VMEM)
SMEM = pl.BlockSpec(memory_space=pltpu.SMEM)
ANY = pl.BlockSpec(memory_space=pl.ANY)
HBM = pl.BlockSpec(memory_space=pltpu.HBM)
SMALL = 12 * 1024 * 1024
LARGE = 40 * 1024 * 1024
UNROLL = 2


def buckets(most):
    pairs = [(4, 6), (5, 7), (6, 8), (8, 10)]
    return [p for p in pairs if max(p) < most] + [(most, most)]


def meta_kernel(n, slots, sub, block_len, sizes, ids, count, live, out, choice, row, rows, send, recv):
    b = lax.axis_index("band")
    c = lax.axis_index("ch")
    half = sub // 2
    row[:, :slots] = ids[...]
    row[:, slots:2 * slots] = jnp.full((1, slots), count[0], jnp.int32)
    row[:, 2 * slots:3 * slots] = jnp.full((1, slots), live[0], jnp.int32)
    row[:, 3 * slots:] = jnp.zeros((1, row.shape[1] - 3 * slots), jnp.int32)
    barrier = pltpu.get_barrier_semaphore()

    def greet(d, carry):
        pl.semaphore_signal(barrier, inc=1, device_id=(lax.rem(b + d, n), c), device_id_type=MESH)
        return carry

    lax.fori_loop(1, n, greet, 0)
    pl.semaphore_wait(barrier, n - 1)

    def copy(d):
        return pltpu.make_async_remote_copy(
            src_ref=row, dst_ref=rows.at[b], send_sem=send.at[d], recv_sem=recv.at[d],
            device_id=(lax.rem(b + d, n), c), device_id_type=MESH,
        )

    def begin(d, carry):
        copy(d).start()
        return carry

    def arrive(d, carry):
        pltpu.make_async_remote_copy(
            src_ref=row, dst_ref=rows.at[lax.rem(b + n - d, n)], send_sem=send.at[d], recv_sem=recv.at[d],
            device_id=(lax.rem(b + d, n), c), device_id_type=MESH,
        ).wait()
        return carry

    lax.fori_loop(1, n, begin, 0)
    rows[b] = row[...]
    lax.fori_loop(1, n, arrive, 0)
    out[...] = rows[...]
    every = rows[:, 0, :]
    named, most, points = every[:, :slots], every[:, slots:2 * slots], every[:, 2 * slots:2 * slots + 1]
    below = jnp.concatenate([points[:1], points[:-1]], axis=0)
    above = jnp.concatenate([points[1:], points[-1:]], axis=0)
    bands = lax.broadcasted_iota(jnp.int32, (n, 1), 0)
    rel = named - bands * sub + half
    rel = jnp.where(lax.broadcasted_iota(jnp.int32, (n, slots), 1) < most, rel, -1)
    counts = []
    for side in range(2):
        total = jnp.zeros((n, 1), F32)
        for i in range(half):
            spot = i if side == 0 else half + sub + i
            hit = jnp.max(jnp.where(rel == spot, 1.0, 0.0), axis=1, keepdims=True)
            alive = (half + i) * block_len < below if side == 0 else i * block_len < above
            total += jnp.where(alive, hit, 0.0)
        counts.append(jnp.max(total, axis=0, keepdims=True))
    pick = jnp.zeros((1, 1), jnp.int32)
    for low, high in sizes[:-1]:
        pick += jnp.where((counts[0] > low) | (counts[1] > high), 1, 0)
    choice[...] = jnp.broadcast_to(pick, choice.shape)


def pack_kernel(n, slots, sub, block_len, meta, grid_ref, out_ref, kind, index, limit, need, rank, mine, place, sem):
    b = lax.axis_index("band")
    core = lax.axis_index("ch")
    half = sub // 2
    width = block_len // 2

    def mark(side, band, owner, flags, ranks, active):
        for i in range(half):
            flags[side, i] = 0
        for k in range(slots):
            rel = meta[band, 0, k] - band * sub + half
            i = rel if side == 0 else rel - half - sub
            inner = rel + half if side == 0 else i
            good = (i >= 0) & (i < half) & (k < meta[band, 0, slots])
            good &= (inner * block_len < meta[owner, 0, 2 * slots]) & active
            i = jnp.clip(i, 0, half - 1)
            flags[side, i] = flags[side, i] | good.astype(jnp.int32)
        run = jnp.int32(0)
        for i in range(half):
            ranks[side, i] = run
            run += flags[side, i]

    up, down = jnp.minimum(b + 1, n - 1), jnp.maximum(b - 1, 0)

    def copy(side, i):
        block = half + i if side == 0 else i
        start = pl.multiple_of((block * 2 + core) * width, width)
        return pltpu.make_async_copy(
            grid_ref.at[:, pl.ds(start, width)], out_ref.at[side, rank[side, i]], sem.at[side, i]
        )

    def each(begin, side):
        for i in range(half):
            @pl.when(need[side, i] > 0)
            def _():
                if begin:
                    copy(side, i).start()
                else:
                    copy(side, i).wait()

    mark(0, up, b, need, rank, b < n - 1)
    each(True, 0)
    mark(1, down, b, need, rank, b > 0)
    each(True, 1)
    mark(0, b, down, mine, place, b > 0)
    mark(1, b, up, mine, place, b < n - 1)
    for k in range(slots):
        rel = meta[b, 0, k] - b * sub + half
        is_low, is_high = rel < half, rel >= half + sub
        side = is_high.astype(jnp.int32)
        i = jnp.clip(jnp.where(is_low, rel, rel - half - sub), 0, half - 1)
        used = k < meta[b, 0, slots]
        outside = is_low | is_high
        far = outside & used & (mine[side, i] > 0)
        owner = jnp.where(is_low, down, jnp.where(is_high, up, b))
        inner = jnp.where(is_low, rel + half, jnp.where(is_high, rel - half - sub, rel - half))
        span = jnp.clip(meta[owner, 0, 2 * slots] - inner * block_len, 0, block_len)
        kind[k] = jnp.where(far, 1 + side, 0)
        local = jnp.clip(rel - half, 0, sub - 1)
        index[k] = jnp.where(far, place[side, i], local)
        limit[k] = jnp.where(used & (far | ~outside), span, 0)
    each(False, 0)
    each(False, 1)


def silu(v):
    return (0.5 * v) * (1.0 + jnp.tanh(0.5 * v))


def layer_kernel(
    n, low, high, chunk, kind, index, limit, pk, grid_h, w_h, emb_h, eo_h, win_h, nin_h, nout_h, src, dst, out,
    rlow, rhigh, loc, wts, blk, part, other, ext, emb, emb_o, eo, eo_o, win, nin, nout,
    init, table, acc, direct, agg, agg_o, give, take, wsem, gsem, lsem, send, recv,
):
    b = lax.axis_index("band")
    c = lax.axis_index("ch")
    sub, channels, width = loc.shape
    slots = w_h.shape[0]
    nodes = part.shape[0]
    half = emb.shape[1]
    up, down = jnp.minimum(b + 1, n - 1), jnp.maximum(b - 1, 0)
    has_up, has_down = b < n - 1, b > 0
    above, below, partner = (up, c), (down, c), (b, 1 - c)
    barrier = pltpu.get_barrier_semaphore()
    pl.semaphore_signal(barrier, inc=1, device_id=partner, device_id_type=MESH)

    @pl.when(has_up)
    def _():
        pl.semaphore_signal(barrier, inc=1, device_id=above, device_id_type=MESH)

    @pl.when(has_down)
    def _():
        pl.semaphore_signal(barrier, inc=1, device_id=below, device_id_type=MESH)

    pl.semaphore_wait(barrier, 1 + has_up.astype(jnp.int32) + has_down.astype(jnp.int32))

    def remote(source, target, k, device):
        return pltpu.make_async_remote_copy(
            src_ref=source, dst_ref=target, send_sem=send.at[k], recv_sem=recv.at[k],
            device_id=device, device_id_type=MESH,
        )

    def neighbours(fwd, bwd):
        def begin():
            pl.when(has_up)(fwd.start)
            pl.when(has_down)(bwd.start)

        def end():
            @pl.when(has_up)
            def _():
                fwd.wait_send()
                bwd.wait_recv()

            @pl.when(has_down)
            def _():
                bwd.wait_send()
                fwd.wait_recv()

        return begin, end

    blocks_begin, blocks_end = neighbours(
        remote(pk.at[0, pl.ds(0, low)], rlow, 0, above), remote(pk.at[1, pl.ds(0, high)], rhigh, 1, below)
    )
    blocks_begin()
    weights = [remote(emb_h, emb_o, 2, partner), remote(eo_h, eo_o, 3, partner)]
    for one in weights:
        one.start()
    off = pl.multiple_of(c * width, width)
    wcopies = [
        pltpu.make_async_copy(w_h.at[k, :, pl.ds(off, width)], wts.at[:, pl.ds(k * width, width)], wsem.at[k])
        for k in range(slots)
    ]
    gcopies = [
        pltpu.make_async_copy(
            grid_h.at[:, pl.ds(pl.multiple_of((2 * i + c) * width, width), width)], loc.at[i], gsem.at[i]
        )
        for i in range(sub)
    ]
    local = [
        pltpu.make_async_copy(x, y, lsem.at[i])
        for i, (x, y) in enumerate(
            [(emb_h, emb), (win_h, win), (eo_h, eo), (nin_h, nin), (nout_h, nout)]
        )
    ]
    for one in wcopies + gcopies + local:
        one.start()

    @pl.when(b == 0)
    def _():
        rlow[...] = jnp.zeros_like(rlow)
        ext[0] = jnp.zeros((nodes, channels), BF16)

    @pl.when(b == n - 1)
    def _():
        rhigh[...] = jnp.zeros_like(rhigh)
        ext[2] = jnp.zeros((nodes, channels), BF16)

    for one in wcopies + gcopies + local + weights:
        one.wait()
    blocks_end()

    column = lax.broadcasted_iota(jnp.int32, (channels, width), 1) + c * width
    for k in range(slots):
        which, i = kind[k], index[k]
        block = jnp.where(which == 1, rlow[jnp.clip(i, 0, low - 1)], loc[i])
        block = jnp.where(which == 2, rhigh[jnp.clip(i, 0, high - 1)], block)
        blk[:, k * width:(k + 1) * width] = jnp.where(column < limit[k], block, jnp.zeros_like(block))
    part[...] = lax.dot_general(wts[...], blk[...], (((1,), (1,)), ((), ())), preferred_element_type=F32)
    swap = remote(part, other, 4, partner)
    swap.start()
    swap.wait()
    ext[1] = (part[...] + other[...]).astype(BF16)
    rows_begin, rows_end = neighbours(remote(ext.at[1], ext.at[0], 5, above), remote(ext.at[1], ext.at[2], 6, below))
    rows_begin()

    mine = pl.ds(pl.multiple_of(c * half, half), half)
    theirs = pl.ds(pl.multiple_of((1 - c) * half, half), half)

    def project(i):
        rem = ext[i]
        init[i, :, mine] = jnp.dot(rem, emb[...], preferred_element_type=F32).astype(BF16)
        init[i, :, theirs] = jnp.dot(rem, emb_o[...], preferred_element_type=F32).astype(BF16)
        source = jnp.dot(init[i], win[0], preferred_element_type=F32)
        table[:, i * nodes:(i + 1) * nodes] = source.T.astype(BF16)

    project(1)
    target = jnp.dot(init[1], win[1], preferred_element_type=F32)
    table[:, 3 * nodes:] = target.T.astype(BF16)
    direct[...] = jnp.dot(init[1], nin[0], preferred_element_type=F32)
    acc[...] = jnp.zeros_like(acc)
    rows_end()
    project(0)
    project(2)

    def step(i, carry):
        cols = pl.ds(pl.multiple_of(i * chunk, chunk), chunk)
        s = src[:, cols] - (b - 1) * nodes
        d = dst[:, cols] - b * nodes
        from_src = lax.broadcasted_iota(jnp.int32, (3 * nodes, chunk), 0) == s
        from_dst = lax.broadcasted_iota(jnp.int32, (nodes, chunk), 0) == d
        hot_src = jnp.where(from_src, 1.0, 0.0).astype(BF16)
        hot_dst = jnp.where(from_dst, 1.0, 0.0).astype(BF16)
        pre = jnp.dot(table[...], jnp.concatenate([hot_src, hot_dst], axis=0), preferred_element_type=F32)
        hidden = silu(pre).astype(BF16)
        acc[...] += lax.dot_general(hot_dst, hidden, (((1,), (1,)), ((), ())), preferred_element_type=F32)
        return carry

    lax.fori_loop(0, src.shape[1] // chunk, step, 0, unroll=UNROLL)
    agg[...] = acc[...].astype(BF16)

    swap = remote(agg, agg_o, 7, partner)
    swap.start()
    own = jnp.dot(agg[...], eo[...], preferred_element_type=F32)
    swap.wait()
    total = (own + jnp.dot(agg_o[...], eo_o[...], preferred_element_type=F32)).astype(BF16)
    update = silu(direct[...] + jnp.dot(total, nin[1], preferred_element_type=F32)).astype(BF16)
    give[...] = jnp.dot(update, nout[:, theirs], preferred_element_type=F32).astype(BF16)
    last = remote(give, take, 8, partner)
    last.start()
    kept = init[1, :, mine].astype(F32) + jnp.dot(update, nout[:, mine], preferred_element_type=F32)
    last.wait()
    out[...] = (kept + take[...].astype(F32)).astype(BF16)


def on_device(
    grid_field, band_points, block_ids, block_count, block_weight, embed_weight,
    edge_src, edge_dst, edge_in_weight, edge_out_weight, node_in_weight, node_out_weight,
):
    n = lax.axis_size("band")
    channels, points = grid_field.shape
    slots, nodes, block_len = block_weight.shape[1:]
    sub = points // block_len
    half = sub // 2
    width = block_len // 2
    hid = embed_weight.shape[1]
    params = lambda limit, **kw: pltpu.CompilerParams(vmem_limit_bytes=limit, **kw)

    sizes = buckets(half)
    meta, choice = pl.pallas_call(
        functools.partial(meta_kernel, n, slots, sub, block_len, sizes),
        out_shape=(
            jax.ShapeDtypeStruct((n, 1, 128), jnp.int32),
            jax.ShapeDtypeStruct((1, 128), jnp.int32),
        ),
        in_specs=[VMEM, SMEM, SMEM], out_specs=(VMEM, VMEM),
        scratch_shapes=[
            pltpu.VMEM((1, 128), jnp.int32),
            pltpu.VMEM((n, 1, 128), jnp.int32),
            pltpu.SemaphoreType.DMA((n,)), pltpu.SemaphoreType.DMA((n,)),
        ],
        compiler_params=params(SMALL, collective_id=len(sizes) + 2, has_side_effects=True),
    )(block_ids, block_count, band_points)

    slot_shape = (2, half, channels, width)
    lists = jax.ShapeDtypeStruct((slots,), jnp.int32)
    table = pltpu.SMEM((2, half), jnp.int32)
    packed, kind, index, limit = pl.pallas_call(
        functools.partial(pack_kernel, n, slots, sub, block_len),
        out_shape=(jax.ShapeDtypeStruct(slot_shape, BF16), lists, lists, lists),
        in_specs=[SMEM, HBM], out_specs=(VMEM, SMEM, SMEM, SMEM),
        scratch_shapes=[table] * 4 + [pltpu.SemaphoreType.DMA((2, half))],
        compiler_params=params(SMALL),
    )(meta, grid_field)

    edges = edge_src.shape[0]
    chunk = max(c for c in (512, 256, 128) if edges % c == 0)

    def layer(i, low, high, *args):
        bf = lambda *shape: pltpu.VMEM(shape, BF16)
        f32 = lambda *shape: pltpu.VMEM(shape, F32)
        return pl.pallas_call(
            functools.partial(layer_kernel, n, low, high, chunk),
            out_shape=jax.ShapeDtypeStruct((nodes, hid), BF16),
            in_specs=[SMEM] * 3 + [ANY] + [HBM] * 7 + [VMEM] * 2, out_specs=VMEM,
            scratch_shapes=[
                bf(low, channels, width), bf(high, channels, width), bf(sub, channels, width),
                bf(nodes, slots * width), bf(channels, slots * width),
                f32(nodes, channels), f32(nodes, channels), bf(3, nodes, channels),
                bf(channels, hid), bf(channels, hid), bf(hid, 2 * hid), bf(hid, 2 * hid),
                bf(2, 2 * hid, hid), bf(2, 2 * hid, hid), bf(hid, 2 * hid),
                bf(3, nodes, 2 * hid), bf(hid, 4 * nodes), f32(nodes, hid), f32(nodes, hid),
                bf(nodes, hid), bf(nodes, hid), bf(nodes, hid), bf(nodes, hid),
                pltpu.SemaphoreType.DMA((slots,)), pltpu.SemaphoreType.DMA((sub,)), pltpu.SemaphoreType.DMA((5,)),
                pltpu.SemaphoreType.DMA((9,)), pltpu.SemaphoreType.DMA((9,)),
            ],
            compiler_params=params(LARGE, collective_id=i, has_side_effects=True),
        )(*args)

    return lax.switch(
        choice[0, 0],
        [functools.partial(layer, i, low, high) for i, (low, high) in enumerate(sizes)],
        kind, index, limit, packed, grid_field, block_weight.reshape(block_weight.shape[1:]), embed_weight, edge_out_weight,
        edge_in_weight, node_in_weight, node_out_weight, edge_src.reshape(1, -1), edge_dst.reshape(1, -1),
    )


def solution(mesh):
    return jax.shard_map(
        on_device,
        mesh=mesh,
        in_specs=(
            P(None, "band"), P("band"), P("band", None), P("band"),
            P("band", None, None, None), P(None, "ch"), P("band"), P("band"),
            P(None, None, "ch"), P("ch", None), P(None, None, "ch"), P("ch", None),
        ),
        out_specs=P("band", "ch"),
        check_vma=False,
    )
```
